32 devices in a mesh: pix: 8 (over z, y), rep: 4 (over x, core).
Axes of the slice: x: 2, y: 2, z: 4, core: 2. Of those that a mesh axis runs over, the one named last changes fastest.
Arguments:
- interferograms: float32 [256, 131072], P(('pix', 'rep')), may hold values from -6 to 6
- epoch_pairs: int32 [2, 256], replicated, may hold values from 0 to 63, as said below
- los: float32 [3, 131072], P(None, ('pix', 'rep')), may hold values from 0.3 to 1
- patch_place: int32 [2, 4096], replicated, may hold values from 0 to 255, as said below
- patch_depth: int32 [4096], replicated, may hold values from 0 to 7
Outputs:
- predicted: float32 [64, 131072], P(None, ('pix', 'rep'))
- slip: float32 [64, 4096], P(None, ('pix', 'rep'))
The draws below stay inside these ranges and needn't reach their ends.
Inputs may be any that keep to these rules, and one draw needn't show every extreme that they name: `epoch_pairs`: row 0 holds an interferogram's earlier epoch and row 1 its later one; the two always differ. `patch_place`: row 0 is an east cell below 256; row 1 is a north cell below 32.
All inputs are finite; a program needn't handle non-finite values.
Results may differ from the reference program's by a relative error of at most 0.0037.
Values may be sent and summed in bfloat16 or wider, within the bound.
A program may use at most 64 MiB of HBM per device.

```python
import jax
import jax.numpy as jnp
from jax import lax

NEP = 64
NIFG = 256
NPATCH = 4096
IMG_W = 1024
SWEEPS = 2
PIX_DEV = 4096
NPIX = 131072
DEVICES = 32


def draw_epoch_pairs(key, part):
    first_key = jax.random.fold_in(key, 11)
    span_key = jax.random.fold_in(key, 12)
    primary = jax.random.randint(first_key, (NIFG,), 0, NEP - 1)
    spread = jax.random.randint(span_key, (NIFG,), 0, 1 << 20)
    secondary = primary + 1 + spread % (NEP - 1 - primary)
    return jnp.stack([primary, secondary]).astype(jnp.int32)


def draw_patch_place(key, part):
    north_cells = max(NPIX // (4 * IMG_W), 1)
    east = jax.random.randint(jax.random.fold_in(key, 31), (NPATCH,), 0, 256)
    north = jax.random.randint(jax.random.fold_in(key, 32), (NPATCH,), 0, north_cells)
    return jnp.stack([east, north]).astype(jnp.int32)


def draw_los(key, part):
    return jax.random.uniform(jax.random.fold_in(key, 41), (3, NPIX), jnp.float32, 0.3, 1.0)


def touch_ends(result, rng, least, high):
    shape = result.shape
    spot = [jax.random.randint(jax.random.fold_in(rng, axis), (), 0, shape[axis]) for axis in range(len(shape))]
    result = result.at[tuple(spot)].set(least)
    longest = shape.index(max(shape))
    spot[longest] = (spot[longest] + 1) % shape[longest]
    return result.at[tuple(spot)].set(high)


def level_of(rng, dims, split, least, high):
    level = 1.0
    for position, parts in split:
        draws = jax.random.uniform(jax.random.fold_in(jax.random.fold_in(rng, 6), position), (parts,), jnp.float32, least / len(split), high / len(split))
        level = level * jnp.repeat(jnp.exp(draws), dims[position] // parts).reshape((-1,) + (1,) * (len(dims) - 1 - position))
    return level


def centred(stream_key, shape, width, limit, cuts=(), kind=jnp.bfloat16):
    level = level_of(stream_key, shape, cuts, -0.22, 0.18) if cuts else 1.0
    values = jax.random.normal(stream_key, shape, jnp.float32) * width * level
    return jnp.minimum(jnp.maximum(values, -limit), limit).astype(kind)


def setup_inputs(seed: int = 0) -> dict:
    streams_of = jax.random.split(jax.random.key(seed), 6)
    return {
        "interferograms": centred(streams_of[0], (NIFG, NPIX), 1.0, 6.0, ((0, 32),), jnp.float32),
        "epoch_pairs": draw_epoch_pairs(jax.random.fold_in(streams_of[5], 71), 0),
        "los": draw_los(jax.random.fold_in(streams_of[5], 71), 0),
        "patch_place": draw_patch_place(jax.random.fold_in(streams_of[5], 71), 0),
        "patch_depth": touch_ends(jax.random.randint(streams_of[4], (NPATCH,), 0, 8), jax.random.fold_in(streams_of[4], 1), 0, 7).astype(jnp.int32),
    }


pixel_step = 0.1
patch_step = 0.4
damping = 0.5
depth_base = 0.5
depth_step = 0.25

def sbas_inverse(epoch_pairs):
    epochs = lax.iota(jnp.int32, NEP)
    design = (epochs[None, :] == epoch_pairs[1][:, None]).astype(jnp.float32) - (epochs[None, :] == epoch_pairs[0][:, None]).astype(jnp.float32)
    normal = jnp.dot(design.T, design, precision=lax.Precision.HIGHEST) + damping * jnp.eye(NEP, dtype=jnp.float32)
    factor = jnp.linalg.cholesky(normal)
    return jax.scipy.linalg.cho_solve((factor, True), design.T)

def green_tile(pixel, los_rows, patch_place, patch_depth):
    column = (pixel % IMG_W).astype(jnp.float32)
    line = (pixel // IMG_W).astype(jnp.float32)
    xpos = (column + 0.5) * pixel_step
    ypos = (line + 0.5) * pixel_step
    patch_x = (patch_place[0].astype(jnp.float32) + 0.5) * patch_step
    patch_y = (patch_place[1].astype(jnp.float32) + 0.5) * patch_step
    patch_z = depth_base + depth_step * patch_depth.astype(jnp.float32)
    delta_x = xpos[:, None] - patch_x[None, :]
    delta_y = ypos[:, None] - patch_y[None, :]
    delta_z = patch_z[None, :]
    dist_sq = delta_x * delta_x + delta_y * delta_y + delta_z * delta_z
    toward = los_rows[0][:, None] * delta_x + los_rows[1][:, None] * delta_y + los_rows[2][:, None] * delta_z
    return (delta_z * toward / (dist_sq * jnp.sqrt(dist_sq))).astype(jnp.bfloat16)

def reference(interferograms, epoch_pairs, los, patch_place, patch_depth):
    pseudo = sbas_inverse(epoch_pairs)
    series = jnp.dot(pseudo.astype(jnp.float32), interferograms.astype(jnp.float32), precision=lax.Precision.HIGHEST, preferred_element_type=jnp.float32)
    total = PIX_DEV * DEVICES
    blocks = total // PIX_DEV
    indices = jnp.arange(blocks, dtype=jnp.int32)

    def tile_at(index):
        start = index * PIX_DEV
        pixel = start + lax.iota(jnp.int32, PIX_DEV)
        los_rows = lax.dynamic_slice_in_dim(los, start, PIX_DEV, 1)
        return (green_tile(pixel, los_rows, patch_place, patch_depth), start)

    def first_step(carry, index):
        rhs, bound = carry
        tile, start = tile_at(index)
        resid = lax.dynamic_slice_in_dim(series, start, PIX_DEV, 1).astype(jnp.bfloat16)
        rhs = rhs + jnp.dot(resid.astype(jnp.float32), tile.astype(jnp.float32), preferred_element_type=jnp.float32)
        magnitude = jnp.abs(tile)
        weight = lax.optimization_barrier(jnp.sum(magnitude.astype(jnp.float32), axis=1)).astype(jnp.bfloat16)
        bound = bound + jnp.dot(weight[None, :].astype(jnp.float32), magnitude.astype(jnp.float32), preferred_element_type=jnp.float32)[0]
        return ((rhs, bound), None)
    zero_rhs = jnp.zeros((NEP, NPATCH), jnp.float32)
    zero_bound = jnp.zeros((NPATCH,), jnp.float32)
    (rhs, bound), unused = lax.scan(first_step, (zero_rhs, zero_bound), indices)
    slip = jnp.zeros((NEP, NPATCH), jnp.float32) + rhs / bound[None, :]
    for sweep in range(1, SWEEPS):
        slip_half = slip.astype(jnp.bfloat16)

        def sweep_step(rhs_now, index):
            tile, start = tile_at(index)
            guess = lax.dot_general(slip_half.astype(jnp.float32), tile.astype(jnp.float32), (((1,), (1,)), ((), ())), preferred_element_type=jnp.float32)
            resid = (lax.dynamic_slice_in_dim(series, start, PIX_DEV, 1) - guess).astype(jnp.bfloat16)
            return (rhs_now + jnp.dot(resid.astype(jnp.float32), tile.astype(jnp.float32), preferred_element_type=jnp.float32), None)
        rhs, unused = lax.scan(sweep_step, zero_rhs, indices)
        slip = slip + rhs / bound[None, :]
    slip_half = slip.astype(jnp.bfloat16)

    def final_block(index):
        tile, start = tile_at(index)
        return lax.dot_general(slip_half.astype(jnp.float32), tile.astype(jnp.float32), (((1,), (1,)), ((), ())), preferred_element_type=jnp.float32)
    pieces = lax.map(final_block, indices)
    predicted = jnp.transpose(pieces, (1, 0, 2)).reshape(NEP, total)
    return (predicted, slip)
```

```python
import functools

import jax
import jax.numpy as jnp
from jax import lax
from jax.experimental import pallas as pl
from jax.experimental.pallas import tpu as pltpu
from jax.sharding import PartitionSpec as P

NEP = 64
IMG_W = 1024
LANES = 128

pixel_step = 0.1
patch_step = 0.4
damping = 0.5
depth_base = 0.5
depth_step = 0.25

F32 = jnp.float32
BF16 = jnp.bfloat16
NT = (((1,), (1,)), ((), ()))
EXTRA = 16


def kernel(
    cfg,
    pairs_ref,
    los_ref,
    place_ref,
    depth_ref,
    xs_ref,
    pred_ref,
    slip_ref,
    pcol_ref,
    prow_ref,
    mat,
    green,
    wacc,
    got,
    series,
    resid,
    bsend,
    bpart,
    send,
    part_a,
    part_b,
    gath_a,
    gath_b,
    full,
    guess,
    stage,
    xsend,
    own,
    half,
    pair_a,
    pair_b,
    s_x,
    r_x,
    r_in,
    s_b,
    r_b,
    s_p,
    r_pa,
    r_pb,
    s_h,
    r_ha,
    r_hb,
    s_g,
    r_ga,
    r_gb,
    s_f,
    r_fa,
    r_fb,
):
    n, reps, npix, npatch, parts, ifg_dev, lines, chunks = cfg
    me = lax.axis_index(("pix", "rep"))
    rep_size = lax.axis_size("rep")
    groups = npatch // LANES
    mine = me // reps
    gathered = n // reps
    split = reps == 1 and n % 8 == 0
    core = me % 2
    chip = me // 2
    partner = me + 1 - 2 * core
    batches = n // 8
    mesh_id = pl.DeviceIdType.MESH

    def ident(d):
        return {"pix": d // rep_size, "rep": d % rep_size}

    def settle(buf, count, sem):
        view = buf.at[pl.ds(0, count)]
        pltpu.make_async_copy(view, view, sem).wait()

    barrier = pltpu.get_barrier_semaphore()

    @pl.loop(1, n)
    def _(k):
        pl.semaphore_signal(
            barrier, inc=1, device_id=ident((me + k) % n), device_id_type=mesh_id
        )

    if chunks > 1:
        loads = r_in.shape[0]
        per_load = n // loads
        wide_load = per_load * npix
        span = npix // chunks
        for i in range(loads):
            pltpu.make_async_copy(
                xs_ref.at[:, pl.ds(i * wide_load, wide_load)],
                stage.at[:, pl.ds(i * wide_load, wide_load)],
                r_in.at[i],
            ).start()
        for i in range(loads):
            pltpu.make_async_copy(
                xs_ref.at[:, pl.ds(i * wide_load, wide_load)],
                stage.at[:, pl.ds(i * wide_load, wide_load)],
                r_in.at[i],
            ).wait()

            @pl.loop(0, per_load)
            def _(j):
                d = i * per_load + j
                for c in range(chunks):
                    at = pl.ds(pl.multiple_of(d * npix + c * span, span), span)
                    xsend[c, d, :, :] = stage[:, at].astype(BF16)

    pl.semaphore_wait(barrier, n - 1)

    for c in range(chunks):

        @pl.loop(1, n)
        def _(k):
            d = (me + k) % n
            pltpu.make_async_remote_copy(
                src_ref=xsend.at[c, d] if chunks > 1 else xs_ref.at[d],
                dst_ref=got.at[c, me],
                send_sem=s_x,
                recv_sem=r_x.at[c],
                device_id=ident(d),
                device_id_type=mesh_id,
            ).start()

    if chunks > 1:
        for c in range(chunks):
            got[c, me, :, :] = xsend[c, me, :, :]
    else:
        own_copy = pltpu.make_async_copy(xs_ref.at[me], got.at[0, me], r_in.at[0])
        own_copy.start()

    patch_x = (place_ref[0:1, :].astype(F32) + 0.5) * patch_step
    patch_y = (place_ref[1:2, :].astype(F32) + 0.5) * patch_step
    depth = depth_base + depth_step * depth_ref[...].astype(F32)
    scale = lax.rsqrt(depth)
    prow_ref[0:1, :] = patch_x
    prow_ref[1:2, :] = scale
    prow_ref[2:3, :] = depth * scale
    for line in range(lines):
        dy = ((me * lines + line).astype(F32) + 0.5) * pixel_step - patch_y
        prow_ref[3 + 2 * line : 4 + 2 * line, :] = dy * scale
        prow_ref[4 + 2 * line : 5 + 2 * line, :] = dy * dy / depth + depth
    pcol_ref[...] = jnp.concatenate([los_ref[...], jnp.zeros((5, npix), F32)], 0).T

    rows = parts * n * ifg_dev
    nifg = n * ifg_dev
    ep = lax.broadcasted_iota(jnp.int32, (NEP, nifg), 0)
    later = (ep == pairs_ref[1:2, :]).astype(F32)
    earlier = (ep == pairs_ref[0:1, :]).astype(F32)
    design = (later - earlier).astype(BF16)
    slot = lax.broadcasted_iota(jnp.int32, (nifg, rows), 1)
    source = slot // (parts * ifg_dev) * ifg_dev + slot % ifg_dev
    spread = (lax.broadcasted_iota(jnp.int32, (nifg, rows), 0) == source).astype(F32).astype(BF16)
    design_half = jnp.dot(design, spread, preferred_element_type=F32).astype(BF16)
    sub = lax.broadcasted_iota(jnp.int32, (NEP, NEP), 0)
    lane = lax.broadcasted_iota(jnp.int32, (NEP, NEP), 1)
    normal = lax.dot_general(design, design, NT, preferred_element_type=F32)
    mat[...] = normal + jnp.where(sub == lane, damping, 0.0)

    def sweep(k):
        m = mat[...]
        col = jnp.sum(jnp.where(lane == k, m, 0.0), axis=1, keepdims=True)
        row = jnp.sum(jnp.where(sub == k, m, 0.0), axis=0, keepdims=True)
        pivot = jnp.sum(jnp.where(lane[0:1] == k, row, 0.0), axis=1, keepdims=True)
        inv = 1.0 / pivot
        scaled = row * inv
        new = m - col * scaled
        new = jnp.where(lane == k, col * inv, new)
        new = jnp.where(sub == k, scaled, new)
        mat[...] = jnp.where((sub == k) & (lane == k), -inv, new)

    strip, wide = 32, 256
    per_line = IMG_W // strip

    for line in range(lines):

        @pl.loop(0, per_line)
        def _(t):
            start = pl.multiple_of(line * IMG_W + t * strip, strip)
            col = pcol_ref[pl.ds(start, strip), :]
            cell = t * strip + lax.broadcasted_iota(jnp.int32, (strip, LANES), 0)
            xpos = (cell.astype(F32) + 0.5) * pixel_step
            east = jnp.broadcast_to(col[:, 0:1], (strip, LANES))
            north = jnp.broadcast_to(col[:, 1:2], (strip, LANES))
            upward = jnp.broadcast_to(col[:, 2:3], (strip, LANES))
            if (line + 1) * per_line <= NEP:
                sweep(line * per_line + t)
            total = jnp.zeros((strip, LANES), F32)
            for c in range(npatch // wide):
                halves = []
                for j in range(wide // LANES):
                    at = slice(c * wide + j * LANES, c * wide + (j + 1) * LANES)
                    u = (xpos - prow_ref[0:1, at]) * prow_ref[1:2, at]
                    r2 = u * u + prow_ref[4 + 2 * line : 5 + 2 * line, at]
                    inv = lax.rsqrt(r2)
                    num = east * u + north * prow_ref[3 + 2 * line : 4 + 2 * line, at]
                    num = num + upward * prow_ref[2:3, at]
                    g = num * (inv * inv * inv)
                    total = total + jnp.abs(g)
                    halves.append(g.astype(BF16))
                green[pl.ds(start, strip), c * wide : (c + 1) * wide] = jnp.concatenate(halves, 1)
            wacc[pl.ds(start, strip), :] = total

    weight = lax.dot_general(
        jnp.ones((EXTRA, LANES), F32),
        wacc[...],
        NT,
        precision=lax.Precision.HIGHEST,
        preferred_element_type=F32,
    ).astype(BF16)
    block = 512

    @pl.loop(0, npatch // block)
    def _(b):
        cols = pl.ds(pl.multiple_of(b * block, block), block)
        row = jnp.dot(weight, jnp.abs(green[:, cols]), preferred_element_type=F32)
        high = row.astype(BF16)
        low = (row - high.astype(F32)).astype(BF16)
        pick = lax.broadcasted_iota(jnp.int32, (EXTRA, block), 0) == 0
        tail = jnp.where(pick, high.astype(F32), low.astype(F32)).astype(BF16)
        for j in range(block // LANES):
            bsend[b * (block // LANES) + j, :, :] = tail[:, j * LANES : (j + 1) * LANES]

    @pl.loop(1, n)
    def _(k):
        d = (me + k) % n
        pltpu.make_async_remote_copy(
            src_ref=bsend.at[d // reps],
            dst_ref=bpart.at[me],
            send_sem=s_b,
            recv_sem=r_b,
            device_id=ident(d),
            device_id_type=mesh_id,
        ).start()

    bpart[me, :, :] = bsend[mine, :, :]

    @pl.loop(min(lines, NEP // per_line) * per_line, NEP)
    def _(k):
        sweep(k)

    inverse = -mat[...]
    inv_hi = inverse.astype(BF16)
    rest = inverse - inv_hi.astype(F32)
    inv_mid = rest.astype(BF16)
    inv_lo = (rest - inv_mid.astype(F32)).astype(BF16)
    pseudo = (
        jnp.dot(inv_hi, design_half, preferred_element_type=F32)
        + jnp.dot(inv_mid, design_half, preferred_element_type=F32)
        + jnp.dot(inv_lo, design_half, preferred_element_type=F32)
    )
    which = (lax.broadcasted_iota(jnp.int32, (NEP, rows), 1) // ifg_dev) % parts

    if chunks == 1:
        own_copy.wait()
    width = npix // parts if chunks == 1 else span
    pieces = []
    for h in range(parts):
        keep = jnp.where(which == h, pseudo, 0.0)
        hi = keep.astype(BF16)
        pieces.append((hi, (keep - hi.astype(F32)).astype(BF16)))

    def solve(c):
        settle(got.at[c], n - 1, r_x.at[c])
        stacked = got[c].reshape(rows, width)
        for h, (hi, lo) in enumerate(pieces):
            piece = jnp.dot(hi, stacked, preferred_element_type=F32)
            piece = piece + jnp.dot(lo, stacked, preferred_element_type=F32)
            at = (c + h) * width
            series[:, at : at + width] = piece
            resid[:, at : at + width] = piece.astype(BF16)

    per_block = block // LANES
    blocks = npatch // block
    first_block = mine // per_block
    side = blocks // 2

    def place(b):
        return (first_block // side + 1 + b // side) % 2 * side + (first_block + 1 + b) % side

    for c in range(chunks - 1):
        solve(c)
        ks = slice(c * span, (c + 1) * span)

        @pl.loop(0, npatch // 1024)
        def _(b):
            cols = pl.ds(pl.multiple_of(b * 1024, 1024), 1024)
            out = jnp.dot(resid[:, ks], green[ks, cols], preferred_element_type=F32)
            if c > 0:
                out = out + guess[:, cols]
            guess[:, cols] = out

    solve(chunks - 1)

    def product(at, first):
        cols = pl.ds(pl.multiple_of(at * block, block), block)
        if first and chunks > 1:
            ks = slice((chunks - 1) * span, npix)
            out = jnp.dot(resid[:, ks], green[ks, cols], preferred_element_type=F32)
            return out + guess[:, cols]
        return jnp.dot(resid[...], green[:, cols], preferred_element_type=F32)

    def bounds():
        settle(bpart, n - 1, r_b)
        settle(bpart, n - 1, s_b)
        both = lax.fori_loop(
            1, n, lambda d, acc: acc + bpart[d].astype(F32), bpart[0].astype(F32)
        )
        return both[0:1] + both[1:2]

    def project(part, recv_sem, pair, pair_sem, first):
        @pl.loop(0, blocks)
        def _(b):
            at = place(b)
            half_out = product(at, first).astype(BF16)
            for j in range(per_block):
                send[at * per_block + j, :, :] = half_out[:, j * LANES : (j + 1) * LANES]
            for j in range(per_block):
                group = at * per_block + j
                for r in range(reps):
                    d = group * reps + r

                    @pl.when(d != me)
                    def _():
                        pltpu.make_async_remote_copy(
                            src_ref=send.at[group],
                            dst_ref=part.at[me],
                            send_sem=s_p,
                            recv_sem=recv_sem,
                            device_id=ident(d),
                            device_id_type=mesh_id,
                        ).start()

        part[me, :, :] = send[mine, :, :]
        settle(part, n - 1, recv_sem)
        settle(part, n - 1, s_p)
        bound = bounds() if first else None
        total = lax.fori_loop(
            1, n, lambda d, acc: acc + part[d].astype(F32), part[0].astype(F32)
        )
        return total, bound

    chips = n // 2
    per_pair = per_block // 2

    def project_split(part, recv_sem, pair, pair_sem, first):
        def forward(at):
            here = pl.ds(at * per_pair, per_pair)
            pltpu.make_async_copy(pair.at[here], pair.at[here], pair_sem.at[at]).wait()
            for j in range(per_pair):
                slot = at * per_pair + j
                send[slot, :, :] = (own[slot] + pair[slot].astype(F32)).astype(BF16)
            for j in range(per_pair):
                slot = at * per_pair + j

                @pl.when(slot != chip)
                def _():
                    pltpu.make_async_remote_copy(
                        src_ref=send.at[slot],
                        dst_ref=part.at[chip],
                        send_sem=s_p,
                        recv_sem=recv_sem,
                        device_id=ident(slot * 2 + core),
                        device_id_type=mesh_id,
                    ).start()

        @pl.loop(0, blocks)
        def _(b):
            at = place(b)
            out = product(at, first)
            for j in range(per_pair):
                even = out[:, 2 * j * LANES : (2 * j + 1) * LANES]
                odd = out[:, (2 * j + 1) * LANES : (2 * j + 2) * LANES]
                slot = at * per_pair + j
                own[slot, :, :] = jnp.where(core == 0, even, odd)
                half[slot, :, :] = jnp.where(core == 0, odd, even).astype(BF16)
            here = pl.ds(at * per_pair, per_pair)
            pltpu.make_async_remote_copy(
                src_ref=half.at[here],
                dst_ref=pair.at[here],
                send_sem=s_h,
                recv_sem=pair_sem.at[at],
                device_id=ident(partner),
                device_id_type=mesh_id,
            ).start()

            @pl.when(b > 0)
            def _():
                forward(place(b - 1))

        forward(place(blocks - 1))
        part[chip, :, :] = send[chip, :, :]
        settle(half, chips, s_h)
        bound = bounds() if first else None
        settle(part, chips - 1, recv_sem)
        settle(part, chips - 1, s_p)
        total = lax.fori_loop(
            1, chips, lambda d, acc: acc + part[d].astype(F32), part[0].astype(F32)
        )
        return total, bound

    tile = 512

    def share(slip, gath, recv_sem, pass_sem, target):
        gath[mine, :, :] = slip.astype(BF16)

        @pl.loop(1, gathered)
        def _(k):
            d = (me + (n - k * reps)) % n
            pltpu.make_async_remote_copy(
                src_ref=gath.at[mine],
                dst_ref=gath.at[mine],
                send_sem=s_g,
                recv_sem=recv_sem.at[first_block],
                device_id=ident(d),
                device_id_type=mesh_id,
            ).start()

        for i in range(blocks):
            at = (first_block + i) % blocks
            settle(gath, per_block - 1 if i == 0 else per_block, recv_sem.at[at])
            for j in range(per_block):
                full[:, j * LANES : (j + 1) * LANES] = gath[at * per_block + j]
            cols = pl.ds(pl.multiple_of(at * block, block), block)

            @pl.loop(0, npix // tile)
            def _(t):
                here = pl.ds(pl.multiple_of(t * tile, tile), tile)
                out = lax.dot_general(
                    full[:, 0:block], green[here, cols], NT, preferred_element_type=F32
                )
                if i > 0:
                    out = target[:, here] + out
                target[:, here] = out

        settle(gath, gathered - 1, s_g)

    def share_split(slip, gath, recv_sem, pass_sem, target):
        mine_at = core * chips + chip
        gath[mine_at, :, :] = slip.astype(BF16)
        each = chips // batches
        home = chip // each

        @pl.loop(1, chips)
        def _(k):
            to = (chip + k) % chips
            pltpu.make_async_remote_copy(
                src_ref=gath.at[mine_at],
                dst_ref=gath.at[mine_at],
                send_sem=s_g,
                recv_sem=recv_sem.at[home],
                device_id=ident(to * 2 + core),
                device_id_type=mesh_id,
            ).start()

        def order(i):
            if batches != 4:
                return (home + i) % batches
            return (home, home + 1 - 2 * (home % 2), (home + 2) % 4, 3 - home)[i]

        def passing(at):
            return pl.ds(core * chips + at * each, each)

        def collect(i):
            at = order(i)
            settle(gath, each - 1 if i == 0 else each, recv_sem.at[at])
            pltpu.make_async_remote_copy(
                src_ref=gath.at[passing(at)],
                dst_ref=gath.at[passing(at)],
                send_sem=s_f,
                recv_sem=pass_sem.at[at],
                device_id=ident(partner),
                device_id_type=mesh_id,
            ).start()

        step = 2 if batches % 2 == 0 else 1
        for i in range(0, batches, step):
            for m in range(step):
                collect(i + m)
            greens = []
            for m in range(step):
                at = order(i + m)
                settle(gath, each, pass_sem.at[at])
                for j in range(each):
                    for p in range(2):
                        lane = (m * 2 * each + 2 * j + p) * LANES
                        full[:, lane : lane + LANES] = gath[p * chips + at * each + j]
                span_at = 2 * each * LANES
                greens.append(pl.ds(pl.multiple_of(at * span_at, span_at), span_at))

            @pl.loop(0, npix // 1024)
            def _(t):
                here = pl.ds(pl.multiple_of(t * 1024, 1024), 1024)
                out = None
                for m in range(step):
                    left = full[:, m * span_at : (m + 1) * span_at]
                    term = lax.dot_general(
                        left, green[here, greens[m]], NT, preferred_element_type=F32
                    )
                    out = term if out is None else out + term
                if i > 0:
                    out = target[:, here] + out
                target[:, here] = out

        settle(gath, chips - 1, s_g)
        settle(gath, chips, s_f)

    if split:
        project, share = project_split, share_split
    sums, bound = project(part_a, r_pa, pair_a, r_ha, True)
    settle(got.at[0], n - 1, s_x)
    for c in range(1, chunks):
        settle(got.at[c], n - 1, s_x)
    slip = sums / bound
    share(slip, gath_a, r_ga, r_fa, guess)
    resid[...] = (series[...] - guess[:, 0:npix]).astype(BF16)
    slip = slip + project(part_b, r_pb, pair_b, r_hb, False)[0] / bound
    slip_ref[...] = slip
    share(slip, gath_b, r_gb, r_fb, pred_ref)


def on_device(interferograms, epoch_pairs, los, patch_place, patch_depth):
    n = lax.axis_size(("pix", "rep"))
    me = lax.axis_index(("pix", "rep"))
    ifg_dev, total = interferograms.shape
    npix = total // n
    npatch = patch_depth.shape[0]
    own = npatch // n
    reps = max(LANES // own, 1)
    parts = max(16 // ifg_dev, 1)
    width = npix // parts
    lines = npix // IMG_W

    chunks = 1
    if ifg_dev % 8 == 0 and lines > 1:
        chunks, parts, width = lines, 1, IMG_W
        xs = interferograms
    else:
        xs = interferograms.astype(BF16).reshape(ifg_dev, n, parts, width)
        xs = xs.transpose(1, 2, 0, 3).reshape(n, parts * ifg_dev, width)
    inside = chunks > 1
    groups = npatch // LANES
    cfg = (n, reps, npix, npatch, parts, ifg_dev, lines, chunks)
    chips = n // 2
    pairs = chips if reps == 1 else 1
    small = (1,) + (16, LANES)
    loads = 8 if n % 8 == 0 else 1
    batches = max(n // 8, 1)
    vmem = pl.BlockSpec(memory_space=pltpu.VMEM)
    piece = (NEP, LANES)
    block = 512
    dma = pltpu.SemaphoreType.DMA
    predicted, slip = pl.pallas_call(
        functools.partial(kernel, cfg),
        out_shape=(
            jax.ShapeDtypeStruct((NEP, npix), F32),
            jax.ShapeDtypeStruct((NEP, LANES), F32),
        ),
        in_specs=[vmem, vmem, vmem, vmem, pl.BlockSpec(memory_space=pl.ANY)],
        out_specs=(vmem, vmem),
        scratch_shapes=[
            pltpu.VMEM((npix, 8), F32),
            pltpu.VMEM((3 + 2 * lines, npatch), F32),
            pltpu.VMEM((NEP, NEP), F32),
            pltpu.VMEM((npix, npatch), BF16),
            pltpu.VMEM((npix, LANES), F32),
            pltpu.VMEM((chunks, n, parts * ifg_dev, width), BF16),
            pltpu.VMEM((NEP, npix), F32),
            pltpu.VMEM((NEP, npix), BF16),
            pltpu.VMEM((groups, EXTRA, LANES), BF16),
            pltpu.VMEM((n, EXTRA, LANES), BF16),
            pltpu.VMEM((groups,) + piece, BF16),
            pltpu.VMEM((n,) + piece, BF16),
            pltpu.VMEM((n,) + piece, BF16),
            pltpu.VMEM((groups, NEP, LANES), BF16),
            pltpu.VMEM((groups, NEP, LANES), BF16),
            pltpu.VMEM((NEP, npatch // 2), BF16),
            pltpu.VMEM((NEP, max(npix, npatch)), F32),
            pltpu.VMEM(interferograms.shape if inside else (8, LANES), F32),
            pltpu.VMEM((chunks, n, ifg_dev, width) if inside else small, BF16),
            pltpu.VMEM((pairs,) + piece, F32),
            pltpu.VMEM((pairs,) + piece, BF16),
            pltpu.VMEM((pairs,) + piece, BF16),
            pltpu.VMEM((pairs,) + piece, BF16),
            dma,
            dma((chunks,)),
            dma((loads,)),
            dma,
            dma,
            dma,
            dma,
            dma,
            dma,
            dma((npatch // block,)),
            dma((npatch // block,)),
            dma,
            dma((max(npatch // block, batches),)),
            dma((max(npatch // block, batches),)),
            dma,
            dma((batches,)),
            dma((batches,)),
        ],
        compiler_params=pltpu.CompilerParams(
            collective_id=0, has_side_effects=True, vmem_limit_bytes=62 * 1024 * 1024
        ),
    )(epoch_pairs, los, patch_place, patch_depth[None], xs)
    if reps > 1:
        slip = lax.dynamic_slice_in_dim(slip, (me % reps) * own, own, 1)
    return (predicted, slip)


def solution(mesh):
    placed = (P(("pix", "rep"), None), P(), P(None, ("pix", "rep")), P(), P())
    return jax.shard_map(
        on_device,
        mesh=mesh,
        in_specs=placed,
        out_specs=(P(None, ("pix", "rep")), P(None, ("pix", "rep"))),
        check_vma=False,
    )
```

```python
import functools

import jax
import jax.numpy as jnp
from jax import lax
from jax.experimental import pallas as pl
from jax.experimental.pallas import tpu as pltpu
from jax.sharding import PartitionSpec as P

NEP = 64
IMG_W = 1024
LANES = 128

damping = 0.5

F32 = jnp.float32
BF16 = jnp.bfloat16
NT = (((1,), (1,)), ((), ()))
EXTRA = 16


def thirds(x):
    high = x.astype(BF16).astype(F32)
    rest = x - high
    mid = rest.astype(BF16).astype(F32)
    return high, mid, (rest - mid).astype(BF16).astype(F32)


def kernel(
    cfg,
    pairs_ref,
    los_ref,
    place_ref,
    depth_ref,
    xs_ref,
    pred_ref,
    slip_ref,
    feat,
    basis,
    prow,
    mat,
    green,
    wacc,
    got,
    series,
    resid,
    bsend,
    bpart,
    send,
    part_a,
    part_b,
    gath_a,
    gath_b,
    full,
    guess,
    stage,
    xsend,
    own,
    half,
    pair_a,
    pair_b,
    s_x,
    r_x,
    r_in,
    s_b,
    r_b,
    s_p,
    r_pa,
    r_pb,
    s_h,
    r_ha,
    r_hb,
    s_g,
    r_ga,
    r_gb,
    s_f,
    r_fa,
    r_fb,
):
    n, reps, npix, npatch, parts, ifg_dev, lines, chunks = cfg
    me = lax.axis_index(("pix", "rep"))
    rep_size = lax.axis_size("rep")
    groups = npatch // LANES
    mine = me // reps
    gathered = n // reps
    split = reps == 1 and n % 8 == 0
    core = me % 2
    chip = me // 2
    partner = me + 1 - 2 * core
    batches = n // 8
    mesh_id = pl.DeviceIdType.MESH

    def ident(d):
        return {"pix": d // rep_size, "rep": d % rep_size}

    def settle(buf, count, sem):
        view = buf.at[pl.ds(0, count)]
        pltpu.make_async_copy(view, view, sem).wait()

    barrier = pltpu.get_barrier_semaphore()

    @pl.loop(1, n)
    def _(k):
        pl.semaphore_signal(
            barrier, inc=1, device_id=ident((me + k) % n), device_id_type=mesh_id
        )

    if chunks > 1:
        loads = r_in.shape[0]
        per_load = n // loads
        wide_load = per_load * npix
        span = npix // chunks
        for i in range(loads):
            pltpu.make_async_copy(
                xs_ref.at[:, pl.ds(i * wide_load, wide_load)],
                stage.at[:, pl.ds(i * wide_load, wide_load)],
                r_in.at[i],
            ).start()
        for i in range(loads):
            pltpu.make_async_copy(
                xs_ref.at[:, pl.ds(i * wide_load, wide_load)],
                stage.at[:, pl.ds(i * wide_load, wide_load)],
                r_in.at[i],
            ).wait()

            @pl.loop(0, per_load)
            def _(j):
                d = i * per_load + j
                for c in range(chunks):
                    at = pl.ds(pl.multiple_of(d * npix + c * span, span), span)
                    xsend[c, d, :, :] = stage[:, at].astype(BF16)

    pixel = lax.broadcasted_iota(jnp.int32, (1, npix), 1)
    odd_x = (2 * (pixel % IMG_W) + 1).astype(F32)
    odd_y = (2 * (me * lines + pixel // IMG_W) + 1).astype(F32)
    cell_x = (8 * place_ref[0:1, :] + 4).astype(F32)
    cell_y = (8 * place_ref[1:2, :] + 4).astype(F32)
    deep = (10 + 5 * depth_ref[...]).astype(F32)
    gain = 20.0 * deep
    left, right = [], []
    for one, values in (
        (los_ref[0:1, :] * odd_x, (gain,)),
        (los_ref[1:2, :] * odd_y, (gain,)),
        (los_ref[0:1, :], thirds(-gain * cell_x)),
        (los_ref[1:2, :], thirds(-gain * cell_y)),
        (los_ref[2:3, :], thirds(gain * deep)[:2]),
    ):
        for a in thirds(one):
            for b in values:
                left.append(a)
                right.append(b)
    spare = feat.shape[1] - len(left)
    left.append(jnp.zeros((spare, npix), F32))
    right.append(jnp.zeros((spare, npatch), F32))
    feat[...] = jnp.concatenate(left, 0).T.astype(BF16)
    basis[...] = jnp.concatenate(right, 0).astype(BF16)
    prow[0:1, :] = cell_x
    for line in range(lines):
        away = (2 * (me * lines + line) + 1).astype(F32) - cell_y
        prow[1 + line : 2 + line, :] = away * away + deep * deep

    pl.semaphore_wait(barrier, n - 1)

    for c in range(chunks):

        @pl.loop(1, n)
        def _(k):
            d = (me + k) % n
            pltpu.make_async_remote_copy(
                src_ref=xsend.at[c, d] if chunks > 1 else xs_ref.at[d],
                dst_ref=got.at[c, me],
                send_sem=s_x,
                recv_sem=r_x.at[c],
                device_id=ident(d),
                device_id_type=mesh_id,
            ).start()

    if chunks > 1:
        for c in range(chunks):
            got[c, me, :, :] = xsend[c, me, :, :]
    else:
        own_copy = pltpu.make_async_copy(xs_ref.at[me], got.at[0, me], r_in.at[0])
        own_copy.start()

    rows = parts * n * ifg_dev
    nifg = n * ifg_dev
    ep = lax.broadcasted_iota(jnp.int32, (NEP, nifg), 0)
    later = (ep == pairs_ref[1:2, :]).astype(F32)
    earlier = (ep == pairs_ref[0:1, :]).astype(F32)
    design = (later - earlier).astype(BF16)
    slot = lax.broadcasted_iota(jnp.int32, (nifg, rows), 1)
    source = slot // (parts * ifg_dev) * ifg_dev + slot % ifg_dev
    spread = (lax.broadcasted_iota(jnp.int32, (nifg, rows), 0) == source).astype(F32).astype(BF16)
    design_half = jnp.dot(design, spread, preferred_element_type=F32).astype(BF16)
    sub = lax.broadcasted_iota(jnp.int32, (NEP, NEP), 0)
    lane = lax.broadcasted_iota(jnp.int32, (NEP, NEP), 1)
    normal = lax.dot_general(design, design, NT, preferred_element_type=F32)
    mat[...] = normal + jnp.where(sub == lane, damping, 0.0)

    def sweep(k):
        m = mat[...]
        col = jnp.sum(jnp.where(lane == k, m, 0.0), axis=1, keepdims=True)
        row = jnp.sum(jnp.where(sub == k, m, 0.0), axis=0, keepdims=True)
        wide_col = jnp.broadcast_to(col, (NEP, NEP))
        pivot = jnp.sum(jnp.where(sub == k, wide_col, 0.0), axis=0, keepdims=True)
        inv = 1.0 / pivot
        scaled = row * inv
        new = m - wide_col * scaled
        new = jnp.where(lane == k, wide_col * inv, new)
        new = jnp.where(sub == k, scaled, new)
        mat[...] = jnp.where((sub == k) & (lane == k), -inv, new)

    strip, wide = 128, 256
    per_line = IMG_W // strip
    turns = 2 * -(-NEP // (lines * per_line))
    swept = min(lines, NEP // (per_line * turns)) * per_line * turns

    def generate(line):
        @pl.loop(0, per_line)
        def _(t):
            start = pl.multiple_of(line * IMG_W + t * strip, strip)
            mix = feat[pl.ds(start, strip), :]
            spot = t * strip + lax.broadcasted_iota(jnp.int32, (strip, LANES), 0)
            xpos = (2 * spot + 1).astype(F32)
            for q in range(turns):
                if (line + 1) * per_line * turns <= swept:
                    sweep((line * per_line + t) * turns + q)
            total = jnp.zeros((strip, LANES), F32)
            for c in range(npatch // wide):
                num = jnp.dot(
                    mix, basis[:, c * wide : (c + 1) * wide], preferred_element_type=F32
                )
                halves = []
                for j in range(wide // LANES):
                    at = slice(c * wide + j * LANES, c * wide + (j + 1) * LANES)
                    away = xpos - prow[0:1, at]
                    inv = lax.rsqrt(away * away + prow[1 + line : 2 + line, at])
                    g = num[:, j * LANES : (j + 1) * LANES] * (inv * inv * inv)
                    total = total + jnp.abs(g)
                    halves.append(g.astype(BF16))
                green[pl.ds(start, strip), c * wide : (c + 1) * wide] = jnp.concatenate(halves, 1)
            wacc[pl.ds(start, strip), :] = total

    for line in range(lines):
        generate(line)

    weight = lax.dot_general(
        jnp.ones((EXTRA, LANES), F32),
        wacc[...],
        NT,
        precision=lax.Precision.HIGHEST,
        preferred_element_type=F32,
    ).astype(BF16)
    block = 512

    @pl.loop(0, npatch // block)
    def _(b):
        cols = pl.ds(pl.multiple_of(b * block, block), block)
        row = jnp.dot(weight, jnp.abs(green[:, cols]), preferred_element_type=F32)
        high = row.astype(BF16)
        low = (row - high.astype(F32)).astype(BF16)
        pick = lax.broadcasted_iota(jnp.int32, (EXTRA, block), 0) == 0
        tail = jnp.where(pick, high.astype(F32), low.astype(F32)).astype(BF16)
        for j in range(block // LANES):
            bsend[b * (block // LANES) + j, :, :] = tail[:, j * LANES : (j + 1) * LANES]

    @pl.loop(1, n)
    def _(k):
        d = (me + k) % n
        pltpu.make_async_remote_copy(
            src_ref=bsend.at[d // reps],
            dst_ref=bpart.at[me],
            send_sem=s_b,
            recv_sem=r_b,
            device_id=ident(d),
            device_id_type=mesh_id,
        ).start()

    bpart[me, :, :] = bsend[mine, :, :]

    @pl.loop(swept, NEP)
    def _(k):
        sweep(k)

    inverse = -mat[...]
    inv_hi = inverse.astype(BF16)
    rest = inverse - inv_hi.astype(F32)
    inv_mid = rest.astype(BF16)
    inv_lo = (rest - inv_mid.astype(F32)).astype(BF16)
    pseudo = (
        jnp.dot(inv_hi, design_half, preferred_element_type=F32)
        + jnp.dot(inv_mid, design_half, preferred_element_type=F32)
        + jnp.dot(inv_lo, design_half, preferred_element_type=F32)
    )
    which = (lax.broadcasted_iota(jnp.int32, (NEP, rows), 1) // ifg_dev) % parts

    if chunks == 1:
        own_copy.wait()
    width = npix // parts if chunks == 1 else span
    pieces = []
    for h in range(parts):
        keep = jnp.where(which == h, pseudo, 0.0)
        hi = keep.astype(BF16)
        pieces.append((hi, (keep - hi.astype(F32)).astype(BF16)))

    def solve(c):
        settle(got.at[c], n - 1, r_x.at[c])
        stacked = got[c].reshape(rows, width)
        for h, (hi, lo) in enumerate(pieces):
            piece = jnp.dot(hi, stacked, preferred_element_type=F32)
            piece = piece + jnp.dot(lo, stacked, preferred_element_type=F32)
            at = (c + h) * width
            series[:, at : at + width] = piece
            resid[:, at : at + width] = piece.astype(BF16)

    per_block = block // LANES
    blocks = npatch // block
    first_block = mine // per_block
    side = blocks // 2

    def place(b):
        return (first_block // side + 1 + b // side) % 2 * side + (first_block + 1 + b) % side

    for c in range(chunks - 1):
        solve(c)
        ks = slice(c * span, (c + 1) * span)

        @pl.loop(0, npatch // 1024)
        def _(b):
            cols = pl.ds(pl.multiple_of(b * 1024, 1024), 1024)
            out = jnp.dot(resid[:, ks], green[ks, cols], preferred_element_type=F32)
            if c > 0:
                out = out + guess[:, cols]
            guess[:, cols] = out

    solve(chunks - 1)

    def product(at, first):
        cols = pl.ds(pl.multiple_of(at * block, block), block)
        if first and chunks > 1:
            ks = slice((chunks - 1) * span, npix)
            out = jnp.dot(resid[:, ks], green[ks, cols], preferred_element_type=F32)
            return out + guess[:, cols]
        return jnp.dot(resid[...], green[:, cols], preferred_element_type=F32)

    def bounds():
        settle(bpart, n - 1, r_b)
        settle(bpart, n - 1, s_b)
        both = lax.fori_loop(
            1, n, lambda d, acc: acc + bpart[d].astype(F32), bpart[0].astype(F32)
        )
        return both[0:1] + both[1:2]

    def project(part, recv_sem, pair, pair_sem, first):
        @pl.loop(0, blocks)
        def _(b):
            at = place(b)
            half_out = product(at, first).astype(BF16)
            for j in range(per_block):
                send[at * per_block + j, :, :] = half_out[:, j * LANES : (j + 1) * LANES]
            for j in range(per_block):
                group = at * per_block + j
                for r in range(reps):
                    d = group * reps + r

                    @pl.when(d != me)
                    def _():
                        pltpu.make_async_remote_copy(
                            src_ref=send.at[group],
                            dst_ref=part.at[me],
                            send_sem=s_p,
                            recv_sem=recv_sem,
                            device_id=ident(d),
                            device_id_type=mesh_id,
                        ).start()

        part[me, :, :] = send[mine, :, :]
        settle(part, n - 1, recv_sem)
        settle(part, n - 1, s_p)
        bound = bounds() if first else None
        total = lax.fori_loop(
            1, n, lambda d, acc: acc + part[d].astype(F32), part[0].astype(F32)
        )
        return total, bound

    chips = n // 2
    per_pair = per_block // 2

    def project_split(part, recv_sem, pair, pair_sem, first):
        def forward(at):
            here = pl.ds(at * per_pair, per_pair)
            pltpu.make_async_copy(pair.at[here], pair.at[here], pair_sem.at[at]).wait()
            for j in range(per_pair):
                slot = at * per_pair + j
                send[slot, :, :] = (own[slot] + pair[slot].astype(F32)).astype(BF16)
            for j in range(per_pair):
                slot = at * per_pair + j

                @pl.when(slot != chip)
                def _():
                    pltpu.make_async_remote_copy(
                        src_ref=send.at[slot],
                        dst_ref=part.at[chip],
                        send_sem=s_p,
                        recv_sem=recv_sem,
                        device_id=ident(slot * 2 + core),
                        device_id_type=mesh_id,
                    ).start()

        @pl.loop(0, blocks)
        def _(b):
            at = place(b)
            out = product(at, first)
            for j in range(per_pair):
                even = out[:, 2 * j * LANES : (2 * j + 1) * LANES]
                odd = out[:, (2 * j + 1) * LANES : (2 * j + 2) * LANES]
                slot = at * per_pair + j
                own[slot, :, :] = jnp.where(core == 0, even, odd)
                half[slot, :, :] = jnp.where(core == 0, odd, even).astype(BF16)
            here = pl.ds(at * per_pair, per_pair)
            pltpu.make_async_remote_copy(
                src_ref=half.at[here],
                dst_ref=pair.at[here],
                send_sem=s_h,
                recv_sem=pair_sem.at[at],
                device_id=ident(partner),
                device_id_type=mesh_id,
            ).start()

            @pl.when(b > 0)
            def _():
                forward(place(b - 1))

        forward(place(blocks - 1))
        part[chip, :, :] = send[chip, :, :]
        settle(half, chips, s_h)
        bound = bounds() if first else None
        settle(part, chips - 1, recv_sem)
        settle(part, chips - 1, s_p)
        total = lax.fori_loop(
            1, chips, lambda d, acc: acc + part[d].astype(F32), part[0].astype(F32)
        )
        return total, bound

    tile = 512

    def share(slip, gath, recv_sem, pass_sem, target):
        gath[mine, :, :] = slip.astype(BF16)

        @pl.loop(1, gathered)
        def _(k):
            d = (me + (n - k * reps)) % n
            pltpu.make_async_remote_copy(
                src_ref=gath.at[mine],
                dst_ref=gath.at[mine],
                send_sem=s_g,
                recv_sem=recv_sem.at[first_block],
                device_id=ident(d),
                device_id_type=mesh_id,
            ).start()

        for i in range(blocks):
            at = (first_block + i) % blocks
            settle(gath, per_block - 1 if i == 0 else per_block, recv_sem.at[at])
            for j in range(per_block):
                full[:, j * LANES : (j + 1) * LANES] = gath[at * per_block + j]
            cols = pl.ds(pl.multiple_of(at * block, block), block)

            @pl.loop(0, npix // tile)
            def _(t):
                here = pl.ds(pl.multiple_of(t * tile, tile), tile)
                out = lax.dot_general(
                    full[:, 0:block], green[here, cols], NT, preferred_element_type=F32
                )
                if i > 0:
                    out = target[:, here] + out
                target[:, here] = out

        settle(gath, gathered - 1, s_g)

    def share_split(slip, gath, recv_sem, pass_sem, target):
        mine_at = core * chips + chip
        gath[mine_at, :, :] = slip.astype(BF16)
        each = chips // batches
        home = chip // each

        @pl.loop(1, chips)
        def _(k):
            to = (chip + k) % chips
            pltpu.make_async_remote_copy(
                src_ref=gath.at[mine_at],
                dst_ref=gath.at[mine_at],
                send_sem=s_g,
                recv_sem=recv_sem.at[home],
                device_id=ident(to * 2 + core),
                device_id_type=mesh_id,
            ).start()

        def order(i):
            if batches != 4:
                return (home + i) % batches
            return (home, home + 1 - 2 * (home % 2), (home + 2) % 4, 3 - home)[i]

        def passing(at):
            return pl.ds(core * chips + at * each, each)

        def collect(i):
            at = order(i)
            settle(gath, each - 1 if i == 0 else each, recv_sem.at[at])
            pltpu.make_async_remote_copy(
                src_ref=gath.at[passing(at)],
                dst_ref=gath.at[passing(at)],
                send_sem=s_f,
                recv_sem=pass_sem.at[at],
                device_id=ident(partner),
                device_id_type=mesh_id,
            ).start()

        step = 2 if batches % 2 == 0 else 1
        for i in range(0, batches, step):
            for m in range(step):
                collect(i + m)
            greens = []
            for m in range(step):
                at = order(i + m)
                settle(gath, each, pass_sem.at[at])
                for j in range(each):
                    for p in range(2):
                        lane = (m * 2 * each + 2 * j + p) * LANES
                        full[:, lane : lane + LANES] = gath[p * chips + at * each + j]
                span_at = 2 * each * LANES
                greens.append(pl.ds(pl.multiple_of(at * span_at, span_at), span_at))

            @pl.loop(0, npix // 1024)
            def _(t):
                here = pl.ds(pl.multiple_of(t * 1024, 1024), 1024)
                out = None
                for m in range(step):
                    left = full[:, m * span_at : (m + 1) * span_at]
                    term = lax.dot_general(
                        left, green[here, greens[m]], NT, preferred_element_type=F32
                    )
                    out = term if out is None else out + term
                if i > 0:
                    out = target[:, here] + out
                target[:, here] = out

        settle(gath, chips - 1, s_g)
        settle(gath, chips, s_f)

    if split:
        project, share = project_split, share_split
    sums, bound = project(part_a, r_pa, pair_a, r_ha, True)
    settle(got.at[0], n - 1, s_x)
    for c in range(1, chunks):
        settle(got.at[c], n - 1, s_x)
    slip = sums / bound
    share(slip, gath_a, r_ga, r_fa, guess)
    resid[...] = (series[...] - guess[:, 0:npix]).astype(BF16)
    slip = slip + project(part_b, r_pb, pair_b, r_hb, False)[0] / bound
    slip_ref[...] = slip
    share(slip, gath_b, r_gb, r_fb, pred_ref)


def on_device(interferograms, epoch_pairs, los, patch_place, patch_depth):
    n = lax.axis_size(("pix", "rep"))
    me = lax.axis_index(("pix", "rep"))
    ifg_dev, total = interferograms.shape
    npix = total // n
    npatch = patch_depth.shape[0]
    own = npatch // n
    reps = max(LANES // own, 1)
    parts = max(16 // ifg_dev, 1)
    width = npix // parts
    lines = npix // IMG_W

    chunks = 1
    if ifg_dev % 8 == 0 and lines > 1:
        chunks, parts, width = lines, 1, IMG_W
        xs = interferograms
    else:
        xs = interferograms.astype(BF16).reshape(ifg_dev, n, parts, width)
        xs = xs.transpose(1, 2, 0, 3).reshape(n, parts * ifg_dev, width)
    inside = chunks > 1
    groups = npatch // LANES
    cfg = (n, reps, npix, npatch, parts, ifg_dev, lines, chunks)
    chips = n // 2
    pairs = chips if reps == 1 else 1
    small = (1,) + (16, LANES)
    loads = 8 if n % 8 == 0 else 1
    batches = max(n // 8, 1)
    vmem = pl.BlockSpec(memory_space=pltpu.VMEM)
    piece = (NEP, LANES)
    block = 512
    dma = pltpu.SemaphoreType.DMA
    predicted, slip = pl.pallas_call(
        functools.partial(kernel, cfg),
        out_shape=(
            jax.ShapeDtypeStruct((NEP, npix), F32),
            jax.ShapeDtypeStruct((NEP, LANES), F32),
        ),
        in_specs=[vmem, vmem, vmem, vmem, pl.BlockSpec(memory_space=pl.ANY)],
        out_specs=(vmem, vmem),
        scratch_shapes=[
            pltpu.VMEM((npix, 32), BF16),
            pltpu.VMEM((32, npatch), BF16),
            pltpu.VMEM((1 + lines, npatch), F32),
            pltpu.VMEM((NEP, NEP), F32),
            pltpu.VMEM((npix, npatch), BF16),
            pltpu.VMEM((npix, LANES), F32),
            pltpu.VMEM((chunks, n, parts * ifg_dev, width), BF16),
            pltpu.VMEM((NEP, npix), F32),
            pltpu.VMEM((NEP, npix), BF16),
            pltpu.VMEM((groups, EXTRA, LANES), BF16),
            pltpu.VMEM((n, EXTRA, LANES), BF16),
            pltpu.VMEM((groups,) + piece, BF16),
            pltpu.VMEM((n,) + piece, BF16),
            pltpu.VMEM((n,) + piece, BF16),
            pltpu.VMEM((groups, NEP, LANES), BF16),
            pltpu.VMEM((groups, NEP, LANES), BF16),
            pltpu.VMEM((NEP, npatch // 2), BF16),
            pltpu.VMEM((NEP, max(npix, npatch)), F32),
            pltpu.VMEM(interferograms.shape if inside else (8, LANES), F32),
            pltpu.VMEM((chunks, n, ifg_dev, width) if inside else small, BF16),
            pltpu.VMEM((pairs,) + piece, F32),
            pltpu.VMEM((pairs,) + piece, BF16),
            pltpu.VMEM((pairs,) + piece, BF16),
            pltpu.VMEM((pairs,) + piece, BF16),
            dma,
            dma((chunks,)),
            dma((loads,)),
            dma,
            dma,
            dma,
            dma,
            dma,
            dma,
            dma((npatch // block,)),
            dma((npatch // block,)),
            dma,
            dma((max(npatch // block, batches),)),
            dma((max(npatch // block, batches),)),
            dma,
            dma((batches,)),
            dma((batches,)),
        ],
        compiler_params=pltpu.CompilerParams(
            collective_id=0, has_side_effects=True, vmem_limit_bytes=62 * 1024 * 1024
        ),
    )(epoch_pairs, los, patch_place, patch_depth[None], xs)
    if reps > 1:
        slip = lax.dynamic_slice_in_dim(slip, (me % reps) * own, own, 1)
    return (predicted, slip)


def solution(mesh):
    placed = (P(("pix", "rep"), None), P(), P(None, ("pix", "rep")), P(), P())
    return jax.shard_map(
        on_device,
        mesh=mesh,
        in_specs=placed,
        out_specs=(P(None, ("pix", "rep")), P(None, ("pix", "rep"))),
        check_vma=False,
    )
```

```python
import functools

import jax
import jax.numpy as jnp
from jax import lax
from jax.experimental import pallas as pl
from jax.experimental.pallas import tpu as pltpu
from jax.sharding import PartitionSpec as P

NEP = 64
IMG_W = 1024
LANES = 128

damping = 0.5

F32 = jnp.float32
BF16 = jnp.bfloat16
NT = (((1,), (1,)), ((), ()))
EXTRA = 16


def thirds(x):
    high = x.astype(BF16).astype(F32)
    rest = x - high
    mid = rest.astype(BF16).astype(F32)
    return high, mid, (rest - mid).astype(BF16).astype(F32)


def kernel(
    cfg,
    pairs_ref,
    los_ref,
    place_ref,
    depth_ref,
    xs_ref,
    pred_ref,
    slip_ref,
    feat,
    basis,
    prow,
    mat,
    green,
    wacc,
    weight,
    brow,
    got,
    series,
    resid,
    bsend,
    bpart,
    send,
    part_a,
    part_b,
    gath_a,
    gath_b,
    full,
    tall,
    guess,
    stage,
    xsend,
    own,
    half,
    pair_a,
    pair_b,
    s_x,
    r_x,
    r_in,
    s_b,
    r_b,
    s_p,
    r_pa,
    r_pb,
    s_h,
    r_ha,
    r_hb,
    s_g,
    r_ga,
    r_gb,
    s_f,
    r_fa,
    r_fb,
):
    n, reps, npix, npatch, parts, ifg_dev, lines, chunks = cfg
    me = lax.axis_index(("pix", "rep"))
    rep_size = lax.axis_size("rep")
    groups = npatch // LANES
    mine = me // reps
    gathered = n // reps
    split = reps == 1 and n % 8 == 0
    core = me % 2
    chip = me // 2
    partner = me + 1 - 2 * core
    batches = n // 8
    mesh_id = pl.DeviceIdType.MESH

    def ident(d):
        return {"pix": d // rep_size, "rep": d % rep_size}

    def settle(buf, count, sem):
        view = buf.at[pl.ds(0, count)]
        pltpu.make_async_copy(view, view, sem).wait()

    barrier = pltpu.get_barrier_semaphore()

    @pl.loop(1, n)
    def _(k):
        pl.semaphore_signal(
            barrier, inc=1, device_id=ident((me + k) % n), device_id_type=mesh_id
        )

    if chunks > 1:
        loads = r_in.shape[0]
        per_load = n // loads
        wide_load = per_load * npix
        span = npix // chunks
        for i in range(loads):
            pltpu.make_async_copy(
                xs_ref.at[:, pl.ds(i * wide_load, wide_load)],
                stage.at[:, pl.ds(i * wide_load, wide_load)],
                r_in.at[i],
            ).start()
        for i in range(loads):
            pltpu.make_async_copy(
                xs_ref.at[:, pl.ds(i * wide_load, wide_load)],
                stage.at[:, pl.ds(i * wide_load, wide_load)],
                r_in.at[i],
            ).wait()

            @pl.loop(0, per_load)
            def _(j):
                d = i * per_load + j
                for c in range(chunks):
                    at = pl.ds(pl.multiple_of(d * npix + c * span, span), span)
                    xsend[c, d, :, :] = stage[:, at].astype(BF16)

    pixel = lax.broadcasted_iota(jnp.int32, (1, npix), 1)
    odd_x = (2 * (pixel % IMG_W) + 1).astype(F32)
    odd_y = (2 * (me * lines + pixel // IMG_W) + 1).astype(F32)
    cell_x = (8 * place_ref[0:1, :] + 4).astype(F32)
    cell_y = (8 * place_ref[1:2, :] + 4).astype(F32)
    deep = (10 + 5 * depth_ref[...]).astype(F32)
    gain = 20.0 * deep
    left, right = [], []
    for one, values in (
        (los_ref[0:1, :] * odd_x, (gain,)),
        (los_ref[1:2, :] * odd_y, (gain,)),
        (los_ref[0:1, :], thirds(-gain * cell_x)),
        (los_ref[1:2, :], thirds(-gain * cell_y)),
        (los_ref[2:3, :], thirds(gain * deep)[:2]),
    ):
        for a in thirds(one):
            for b in values:
                left.append(a)
                right.append(b)
    spare = feat.shape[1] - len(left)
    left.append(jnp.zeros((spare, npix), F32))
    right.append(jnp.zeros((spare, npatch), F32))
    feat[...] = jnp.concatenate(left, 0).T.astype(BF16)
    basis[...] = jnp.concatenate(right, 0).astype(BF16)
    prow[0:1, :] = cell_x
    for line in range(lines):
        away = (2 * (me * lines + line) + 1).astype(F32) - cell_y
        prow[1 + line : 2 + line, :] = away * away + deep * deep

    pl.semaphore_wait(barrier, n - 1)

    for c in range(chunks):

        @pl.loop(1, n)
        def _(k):
            d = (me + k) % n
            pltpu.make_async_remote_copy(
                src_ref=xsend.at[c, d] if chunks > 1 else xs_ref.at[d],
                dst_ref=got.at[c, me],
                send_sem=s_x,
                recv_sem=r_x.at[c],
                device_id=ident(d),
                device_id_type=mesh_id,
            ).start()

    if chunks > 1:
        for c in range(chunks):
            got[c, me, :, :] = xsend[c, me, :, :]
    else:
        own_copy = pltpu.make_async_copy(xs_ref.at[me], got.at[0, me], r_in.at[0])
        own_copy.start()

    rows = parts * n * ifg_dev
    nifg = n * ifg_dev
    ep = lax.broadcasted_iota(jnp.int32, (NEP, nifg), 0)
    later = (ep == pairs_ref[1:2, :]).astype(F32)
    earlier = (ep == pairs_ref[0:1, :]).astype(F32)
    design = (later - earlier).astype(BF16)
    slot = lax.broadcasted_iota(jnp.int32, (nifg, rows), 1)
    source = slot // (parts * ifg_dev) * ifg_dev + slot % ifg_dev
    spread = (lax.broadcasted_iota(jnp.int32, (nifg, rows), 0) == source).astype(F32).astype(BF16)
    design_half = jnp.dot(design, spread, preferred_element_type=F32).astype(BF16)
    sub = lax.broadcasted_iota(jnp.int32, (NEP, NEP), 0)
    lane = lax.broadcasted_iota(jnp.int32, (NEP, NEP), 1)
    normal = lax.dot_general(design, design, NT, preferred_element_type=F32)
    mat[...] = normal + jnp.where(sub == lane, damping, 0.0)

    def sweep(k):
        m = mat[...]
        col = jnp.sum(jnp.where(lane == k, m, 0.0), axis=1, keepdims=True)
        row = jnp.sum(jnp.where(sub == k, m, 0.0), axis=0, keepdims=True)
        wide_col = jnp.broadcast_to(col, (NEP, NEP))
        pivot = jnp.sum(jnp.where(sub == k, wide_col, 0.0), axis=0, keepdims=True)
        inv = 1.0 / pivot
        scaled = row * inv
        new = m - wide_col * scaled
        new = jnp.where(lane == k, wide_col * inv, new)
        new = jnp.where(sub == k, scaled, new)
        mat[...] = jnp.where((sub == k) & (lane == k), -inv, new)

    strip, wide = 128, 256
    per_line = IMG_W // strip
    turns = 2 * -(-NEP // (lines * per_line))
    swept = min(lines, NEP // (per_line * turns)) * per_line * turns

    slab = npatch // per_line

    def weigh(line):
        here = slice(line * IMG_W, (line + 1) * IMG_W)
        weight[...] = lax.dot_general(
            jnp.ones((EXTRA, LANES), F32),
            wacc[here, :],
            NT,
            precision=lax.Precision.HIGHEST,
            preferred_element_type=F32,
        ).astype(BF16)

    def gather_bound(line, t):
        here = slice(line * IMG_W, (line + 1) * IMG_W)
        cols = pl.ds(pl.multiple_of(t * slab, slab), slab)
        row = jnp.dot(weight[...], jnp.abs(green[here, cols]), preferred_element_type=F32)
        if line > 0:
            row = row + brow[:, cols]
        brow[:, cols] = row

    def generate(line):
        if line > 0:
            weigh(line - 1)

        @pl.loop(0, per_line)
        def _(t):
            if line > 0:
                gather_bound(line - 1, t)
            start = pl.multiple_of(line * IMG_W + t * strip, strip)
            mix = feat[pl.ds(start, strip), :]
            spot = t * strip + lax.broadcasted_iota(jnp.int32, (strip, LANES), 0)
            xpos = (2 * spot + 1).astype(F32)
            for q in range(turns):
                if (line + 1) * per_line * turns <= swept:
                    sweep((line * per_line + t) * turns + q)
            total = jnp.zeros((strip, LANES), F32)
            for c in range(npatch // wide):
                num = jnp.dot(
                    mix, basis[:, c * wide : (c + 1) * wide], preferred_element_type=F32
                )
                halves = []
                for j in range(wide // LANES):
                    at = slice(c * wide + j * LANES, c * wide + (j + 1) * LANES)
                    away = xpos - prow[0:1, at]
                    inv = lax.rsqrt(away * away + prow[1 + line : 2 + line, at])
                    g = num[:, j * LANES : (j + 1) * LANES] * (inv * inv * inv)
                    total = total + jnp.abs(g)
                    halves.append(g.astype(BF16))
                green[pl.ds(start, strip), c * wide : (c + 1) * wide] = jnp.concatenate(halves, 1)
            wacc[pl.ds(start, strip), :] = total

    for line in range(lines):
        generate(line)

    block = 512
    weigh(lines - 1)

    @pl.loop(0, npatch // slab)
    def _(b):
        gather_bound(lines - 1, b)
        row = brow[:, pl.ds(pl.multiple_of(b * slab, slab), slab)]
        high = row.astype(BF16)
        low = (row - high.astype(F32)).astype(BF16)
        pick = lax.broadcasted_iota(jnp.int32, (EXTRA, slab), 0) == 0
        tail = jnp.where(pick, high.astype(F32), low.astype(F32)).astype(BF16)
        for j in range(slab // LANES):
            bsend[b * (slab // LANES) + j, :, :] = tail[:, j * LANES : (j + 1) * LANES]

    @pl.loop(1, n)
    def _(k):
        d = (me + k) % n
        pltpu.make_async_remote_copy(
            src_ref=bsend.at[d // reps],
            dst_ref=bpart.at[me],
            send_sem=s_b,
            recv_sem=r_b,
            device_id=ident(d),
            device_id_type=mesh_id,
        ).start()

    bpart[me, :, :] = bsend[mine, :, :]

    @pl.loop(swept, NEP)
    def _(k):
        sweep(k)

    inverse = -mat[...]
    inv_hi = inverse.astype(BF16)
    rest = inverse - inv_hi.astype(F32)
    inv_mid = rest.astype(BF16)
    inv_lo = (rest - inv_mid.astype(F32)).astype(BF16)
    pseudo = (
        jnp.dot(inv_hi, design_half, preferred_element_type=F32)
        + jnp.dot(inv_mid, design_half, preferred_element_type=F32)
        + jnp.dot(inv_lo, design_half, preferred_element_type=F32)
    )
    which = (lax.broadcasted_iota(jnp.int32, (NEP, rows), 1) // ifg_dev) % parts

    if chunks == 1:
        own_copy.wait()
    width = npix // parts if chunks == 1 else span
    pieces = []
    for h in range(parts):
        keep = jnp.where(which == h, pseudo, 0.0)
        hi = keep.astype(BF16)
        pieces.append((hi, (keep - hi.astype(F32)).astype(BF16)))

    def solve(c):
        settle(got.at[c], n - 1, r_x.at[c])
        stacked = got[c].reshape(rows, width)
        for h, (hi, lo) in enumerate(pieces):
            piece = jnp.dot(hi, stacked, preferred_element_type=F32)
            piece = piece + jnp.dot(lo, stacked, preferred_element_type=F32)
            at = (c + h) * width
            series[:, at : at + width] = piece
            resid[:, at : at + width] = piece.astype(BF16)

    per_block = block // LANES
    blocks = npatch // block
    first_block = mine // per_block
    side = blocks // 2

    def place(b):
        return (first_block // side + 1 + b // side) % 2 * side + (first_block + 1 + b) % side

    for c in range(chunks - 1):
        solve(c)
        ks = slice(c * span, (c + 1) * span)

        @pl.loop(0, npatch // 1024)
        def _(b):
            cols = pl.ds(pl.multiple_of(b * 1024, 1024), 1024)
            out = jnp.dot(resid[:, ks], green[ks, cols], preferred_element_type=F32)
            if c > 0:
                out = out + guess[:, cols]
            guess[:, cols] = out

    solve(chunks - 1)

    def product(at, first):
        cols = pl.ds(pl.multiple_of(at * block, block), block)
        if first and chunks > 1:
            ks = slice((chunks - 1) * span, npix)
            out = jnp.dot(resid[:, ks], green[ks, cols], preferred_element_type=F32)
            return out + guess[:, cols]
        return jnp.dot(resid[...], green[:, cols], preferred_element_type=F32)

    def bounds():
        settle(bpart, n - 1, r_b)
        settle(bpart, n - 1, s_b)
        both = lax.fori_loop(
            1, n, lambda d, acc: acc + bpart[d].astype(F32), bpart[0].astype(F32)
        )
        return both[0:1] + both[1:2]

    def project(part, recv_sem, pair, pair_sem, first):
        @pl.loop(0, blocks)
        def _(b):
            at = place(b)
            half_out = product(at, first).astype(BF16)
            for j in range(per_block):
                send[at * per_block + j, :, :] = half_out[:, j * LANES : (j + 1) * LANES]
            for j in range(per_block):
                group = at * per_block + j
                for r in range(reps):
                    d = group * reps + r

                    @pl.when(d != me)
                    def _():
                        pltpu.make_async_remote_copy(
                            src_ref=send.at[group],
                            dst_ref=part.at[me],
                            send_sem=s_p,
                            recv_sem=recv_sem,
                            device_id=ident(d),
                            device_id_type=mesh_id,
                        ).start()

        part[me, :, :] = send[mine, :, :]
        settle(part, n - 1, recv_sem)
        settle(part, n - 1, s_p)
        bound = bounds() if first else None
        total = lax.fori_loop(
            1, n, lambda d, acc: acc + part[d].astype(F32), part[0].astype(F32)
        )
        return total, bound

    chips = n // 2
    per_pair = per_block // 2

    def project_split(part, recv_sem, pair, pair_sem, first):
        def forward(at):
            here = pl.ds(at * per_pair, per_pair)
            pltpu.make_async_copy(pair.at[here], pair.at[here], pair_sem.at[at]).wait()
            for j in range(per_pair):
                slot = at * per_pair + j
                send[slot, :, :] = (own[slot] + pair[slot].astype(F32)).astype(BF16)
            for j in range(per_pair):
                slot = at * per_pair + j

                @pl.when(slot != chip)
                def _():
                    pltpu.make_async_remote_copy(
                        src_ref=send.at[slot],
                        dst_ref=part.at[chip],
                        send_sem=s_p,
                        recv_sem=recv_sem,
                        device_id=ident(slot * 2 + core),
                        device_id_type=mesh_id,
                    ).start()

        @pl.loop(0, blocks)
        def _(b):
            at = place(b)
            out = product(at, first)
            for j in range(per_pair):
                even = out[:, 2 * j * LANES : (2 * j + 1) * LANES]
                odd = out[:, (2 * j + 1) * LANES : (2 * j + 2) * LANES]
                slot = at * per_pair + j
                own[slot, :, :] = jnp.where(core == 0, even, odd)
                half[slot, :, :] = jnp.where(core == 0, odd, even).astype(BF16)
            here = pl.ds(at * per_pair, per_pair)
            pltpu.make_async_remote_copy(
                src_ref=half.at[here],
                dst_ref=pair.at[here],
                send_sem=s_h,
                recv_sem=pair_sem.at[at],
                device_id=ident(partner),
                device_id_type=mesh_id,
            ).start()

            @pl.when(b > 0)
            def _():
                forward(place(b - 1))

        forward(place(blocks - 1))
        part[chip, :, :] = send[chip, :, :]
        settle(half, chips, s_h)
        bound = bounds() if first else None
        settle(part, chips - 1, recv_sem)
        settle(part, chips - 1, s_p)
        total = lax.fori_loop(
            1, chips, lambda d, acc: acc + part[d].astype(F32), part[0].astype(F32)
        )
        return total, bound

    tile = 512

    def share(slip, gath, recv_sem, pass_sem, target):
        gath[mine, :, :] = slip.astype(BF16)

        @pl.loop(1, gathered)
        def _(k):
            d = (me + (n - k * reps)) % n
            pltpu.make_async_remote_copy(
                src_ref=gath.at[mine],
                dst_ref=gath.at[mine],
                send_sem=s_g,
                recv_sem=recv_sem.at[first_block],
                device_id=ident(d),
                device_id_type=mesh_id,
            ).start()

        for i in range(blocks):
            at = (first_block + i) % blocks
            settle(gath, per_block - 1 if i == 0 else per_block, recv_sem.at[at])
            for j in range(per_block):
                full[:, j * LANES : (j + 1) * LANES] = gath[at * per_block + j]
            cols = pl.ds(pl.multiple_of(at * block, block), block)

            @pl.loop(0, npix // tile)
            def _(t):
                here = pl.ds(pl.multiple_of(t * tile, tile), tile)
                out = lax.dot_general(
                    full[:, 0:block], green[here, cols], NT, preferred_element_type=F32
                )
                if i > 0:
                    out = target[:, here] + out
                target[:, here] = out

        settle(gath, gathered - 1, s_g)

    each = chips // batches
    home = chip // each
    span_at = 2 * each * LANES

    def share_split(slip, gath, recv_sem, pass_sem, target):
        mine_at = core * chips + chip
        gath[mine_at, :, :] = slip.astype(BF16)

        def give(to, side_core):
            pltpu.make_async_remote_copy(
                src_ref=gath.at[mine_at],
                dst_ref=gath.at[mine_at],
                send_sem=s_g,
                recv_sem=recv_sem.at[home],
                device_id=ident(to * 2 + side_core),
                device_id_type=mesh_id,
            ).start()

        give(chip, 1 - core)
        for k in range(1, each):
            to = home * each + (chip + k) % each
            give(to, core)
            give(to, 1 - core)

        def order(i):
            if batches != 4:
                return (home + i) % batches
            low, high = i % 2, i // 2
            bit = home % 2
            near = bit + low - 2 * bit * low
            far = home // 2 + high - 2 * (home // 2) * high
            return 2 * far + near

        @pl.loop(1, batches)
        def _(i):
            for k in range(each):
                give(order(i) * each + (chip + k) % each, core)

        def passing(at):
            return pl.ds(core * chips + at * each, each)

        def collect(i):
            at = order(i)
            settle(gath, each, recv_sem.at[at])
            pltpu.make_async_remote_copy(
                src_ref=gath.at[passing(at)],
                dst_ref=gath.at[passing(at)],
                send_sem=s_f,
                recv_sem=pass_sem.at[at],
                device_id=ident(partner),
                device_id_type=mesh_id,
            ).start()

        target[:, 0:npix] = jnp.zeros((NEP, npix), F32)
        groups_in = 4
        rounds = npix // (1024 * groups_in)

        @pl.loop(0, batches)
        def _(i):
            at = order(i)

            @pl.when(i == 0)
            def _():
                settle(gath, 2 * each - 1, recv_sem.at[at])

            @pl.when(i > 0)
            def _():
                settle(gath, each, pass_sem.at[at])

            for j in range(each):
                for p in range(2):
                    lane = (2 * j + p) * LANES
                    full[:, lane : lane + LANES] = gath[p * chips + at * each + j]
            tall[...] = full[:, 0:span_at].T

            @pl.loop(0, rounds)
            def _(trip):
                @pl.when((i + 1 < batches) & (trip == rounds // 2))
                def _():
                    collect(i + 1)

                for sub_trip in range(groups_in):
                    start = (trip * groups_in + sub_trip) * 1024
                    flat = pl.ds(pl.multiple_of(start, 512), 512)
                    long = pl.ds(pl.multiple_of(start + 512, 512), 512)
                    wide_out = long_out = None
                    for k in range(0, span_at, 256):
                        ks = slice(k, k + 256)
                        cols = pl.ds(pl.multiple_of(at * span_at + k, 256), 256)
                        a = lax.dot_general(
                            full[:, ks], green[flat, cols], NT, preferred_element_type=F32
                        )
                        b = jnp.dot(green[long, cols], tall[ks, :], preferred_element_type=F32)
                        wide_out = a if wide_out is None else wide_out + a
                        long_out = b if long_out is None else long_out + b
                    target[:, flat] = target[:, flat] + wide_out
                    target[:, long] = target[:, long] + long_out.T

        settle(gath, 2 * each - 1 + (batches - 1) * each, s_g)
        settle(gath, (batches - 1) * each, s_f)

    if split:
        project, share = project_split, share_split
    sums, bound = project(part_a, r_pa, pair_a, r_ha, True)
    settle(got.at[0], n - 1, s_x)
    for c in range(1, chunks):
        settle(got.at[c], n - 1, s_x)
    slip = sums / bound
    share(slip, gath_a, r_ga, r_fa, guess)
    resid[...] = (series[...] - guess[:, 0:npix]).astype(BF16)
    slip = slip + project(part_b, r_pb, pair_b, r_hb, False)[0] / bound
    slip_ref[...] = slip
    share(slip, gath_b, r_gb, r_fb, pred_ref)


def relay(pred_ref, slip_ref, pred_out, slip_out, pred_buf, slip_buf, sems):
    rows = 8
    count = pred_ref.shape[0] // rows
    moves = [(slip_ref, slip_buf, slip_out)]
    for i in range(count):
        at = pl.ds(i * rows, rows)
        moves.append((pred_ref.at[at], pred_buf.at[at], pred_out.at[at]))
    loads = [pltpu.make_async_copy(a, b, sems.at[0, i]) for i, (a, b, c) in enumerate(moves)]
    stores = [pltpu.make_async_copy(b, c, sems.at[1, i]) for i, (a, b, c) in enumerate(moves)]
    for load in loads:
        load.start()
    for load, store in zip(loads, stores):
        load.wait()
        store.start()
    for store in stores:
        store.wait()


def on_device(interferograms, epoch_pairs, los, patch_place, patch_depth):
    n = lax.axis_size(("pix", "rep"))
    me = lax.axis_index(("pix", "rep"))
    ifg_dev, total = interferograms.shape
    npix = total // n
    npatch = patch_depth.shape[0]
    own = npatch // n
    reps = max(LANES // own, 1)
    parts = max(16 // ifg_dev, 1)
    width = npix // parts
    lines = npix // IMG_W

    chunks = 1
    if ifg_dev % 8 == 0 and lines > 1:
        chunks, parts, width = lines, 1, IMG_W
        xs = interferograms
    else:
        xs = interferograms.astype(BF16).reshape(ifg_dev, n, parts, width)
        xs = xs.transpose(1, 2, 0, 3).reshape(n, parts * ifg_dev, width)
    inside = chunks > 1
    groups = npatch // LANES
    cfg = (n, reps, npix, npatch, parts, ifg_dev, lines, chunks)
    chips = n // 2
    pairs = chips if reps == 1 else 1
    small = (1,) + (16, LANES)
    loads = 8 if n % 8 == 0 else 1
    batches = max(n // 8, 1)
    vmem = pl.BlockSpec(memory_space=pltpu.VMEM)
    piece = (NEP, LANES)
    block = 512
    dma = pltpu.SemaphoreType.DMA
    predicted, slip = pl.pallas_call(
        functools.partial(kernel, cfg),
        out_shape=(
            jax.ShapeDtypeStruct((NEP, npix), F32),
            jax.ShapeDtypeStruct((NEP, LANES), F32),
        ),
        in_specs=[vmem, vmem, vmem, vmem, pl.BlockSpec(memory_space=pl.ANY)],
        out_specs=(vmem, vmem),
        scratch_shapes=[
            pltpu.VMEM((npix, 32), BF16),
            pltpu.VMEM((32, npatch), BF16),
            pltpu.VMEM((1 + lines, npatch), F32),
            pltpu.VMEM((NEP, NEP), F32),
            pltpu.VMEM((npix, npatch), BF16),
            pltpu.VMEM((npix, LANES), F32),
            pltpu.VMEM((EXTRA, IMG_W), BF16),
            pltpu.VMEM((EXTRA, npatch), F32),
            pltpu.VMEM((chunks, n, parts * ifg_dev, width), BF16),
            pltpu.VMEM((NEP, npix), F32),
            pltpu.VMEM((NEP, npix), BF16),
            pltpu.VMEM((groups, EXTRA, LANES), BF16),
            pltpu.VMEM((n, EXTRA, LANES), BF16),
            pltpu.VMEM((groups,) + piece, BF16),
            pltpu.VMEM((n,) + piece, BF16),
            pltpu.VMEM((n,) + piece, BF16),
            pltpu.VMEM((groups, NEP, LANES), BF16),
            pltpu.VMEM((groups, NEP, LANES), BF16),
            pltpu.VMEM((NEP, max(block, 2 * LANES * chips // batches)), BF16),
            pltpu.VMEM((2 * LANES * chips // batches, NEP), BF16),
            pltpu.VMEM((NEP, max(npix, npatch)), F32),
            pltpu.VMEM(interferograms.shape if inside else (8, LANES), F32),
            pltpu.VMEM((chunks, n, ifg_dev, width) if inside else small, BF16),
            pltpu.VMEM((pairs,) + piece, F32),
            pltpu.VMEM((pairs,) + piece, BF16),
            pltpu.VMEM((pairs,) + piece, BF16),
            pltpu.VMEM((pairs,) + piece, BF16),
            dma,
            dma((chunks,)),
            dma((loads,)),
            dma,
            dma,
            dma,
            dma,
            dma,
            dma,
            dma((npatch // block,)),
            dma((npatch // block,)),
            dma,
            dma((max(npatch // block, batches),)),
            dma((max(npatch // block, batches),)),
            dma,
            dma((batches,)),
            dma((batches,)),
        ],
        compiler_params=pltpu.CompilerParams(
            collective_id=0, has_side_effects=True, vmem_limit_bytes=62 * 1024 * 1024
        ),
    )(epoch_pairs, los, patch_place, patch_depth[None], xs)
    anywhere = pl.BlockSpec(memory_space=pl.ANY)
    predicted, slip = pl.pallas_call(
        relay,
        out_shape=tuple(jax.ShapeDtypeStruct(a.shape, F32) for a in (predicted, slip)),
        in_specs=[anywhere, anywhere],
        out_specs=(anywhere, anywhere),
        scratch_shapes=[
            pltpu.VMEM(predicted.shape, F32),
            pltpu.VMEM(slip.shape, F32),
            dma((2, 1 + NEP // 8)),
        ],
    )(predicted, slip)
    if reps > 1:
        slip = lax.dynamic_slice_in_dim(slip, (me % reps) * own, own, 1)
    return (predicted, slip)


def solution(mesh):
    placed = (P(("pix", "rep"), None), P(), P(None, ("pix", "rep")), P(), P())
    return jax.shard_map(
        on_device,
        mesh=mesh,
        in_specs=placed,
        out_specs=(P(None, ("pix", "rep")), P(None, ("pix", "rep"))),
        check_vma=False,
    )
```

```python
import functools

import jax
import jax.numpy as jnp
from jax import lax
from jax.experimental import pallas as pl
from jax.experimental.pallas import tpu as pltpu
from jax.sharding import PartitionSpec as P

NEP = 64
IMG_W = 1024
LANES = 128

damping = 0.5

F32 = jnp.float32
BF16 = jnp.bfloat16
NT = (((1,), (1,)), ((), ()))
EXTRA = 16


def thirds(x):
    high = x.astype(BF16).astype(F32)
    rest = x - high
    mid = rest.astype(BF16).astype(F32)
    return high, mid, (rest - mid).astype(BF16).astype(F32)


def kernel(
    cfg,
    pairs_ref,
    los_ref,
    place_ref,
    depth_ref,
    xs_ref,
    pred_ref,
    slip_ref,
    feat,
    basis,
    prow,
    mat,
    green,
    wacc,
    weight,
    brow,
    got,
    series,
    resid,
    bsend,
    bpart,
    send,
    part_a,
    part_b,
    gath_a,
    gath_b,
    full,
    tall,
    guess,
    stage,
    xsend,
    over,
    back,
    own,
    half,
    pair_a,
    pair_b,
    s_x,
    r_x,
    r_in,
    s_m,
    r_m,
    s_b,
    r_b,
    s_p,
    r_pa,
    r_pb,
    s_h,
    r_ha,
    r_hb,
    s_g,
    r_ga,
    r_gb,
    s_f,
    r_fa,
    r_fb,
):
    n, reps, npix, npatch, parts, ifg_dev, lines, chunks = cfg
    me = lax.axis_index(("pix", "rep"))
    rep_size = lax.axis_size("rep")
    groups = npatch // LANES
    mine = me // reps
    gathered = n // reps
    split = reps == 1 and n % 8 == 0
    core = me % 2
    chip = me // 2
    partner = me + 1 - 2 * core
    batches = n // 8
    many = n // 2
    slot_me = me % many
    half_me = me // many
    mirror = (me + many) % n
    mesh_id = pl.DeviceIdType.MESH

    def ident(d):
        return {"pix": d // rep_size, "rep": d % rep_size}

    def settle(buf, count, sem):
        view = buf.at[pl.ds(0, count)]
        pltpu.make_async_copy(view, view, sem).wait()

    barrier = pltpu.get_barrier_semaphore()

    @pl.loop(1, n)
    def _(k):
        pl.semaphore_signal(
            barrier, inc=1, device_id=ident((me + k) % n), device_id_type=mesh_id
        )

    if chunks > 1:
        loads = r_in.shape[0]
        per_load = n // loads
        wide_load = per_load * npix
        span = npix // chunks
        for i in range(loads):
            pltpu.make_async_copy(
                xs_ref.at[:, pl.ds(i * wide_load, wide_load)],
                stage.at[:, pl.ds(i * wide_load, wide_load)],
                r_in.at[i],
            ).start()

    pixel = lax.broadcasted_iota(jnp.int32, (1, npix), 1)
    odd_x = (2 * (pixel % IMG_W) + 1).astype(F32)
    odd_y = (2 * (me * lines + pixel // IMG_W) + 1).astype(F32)
    cell_x = (8 * place_ref[0:1, :] + 4).astype(F32)
    cell_y = (8 * place_ref[1:2, :] + 4).astype(F32)
    deep = (10 + 5 * depth_ref[...]).astype(F32)
    gain = 20.0 * deep
    left, right = [], []
    for one, values in (
        (los_ref[0:1, :] * odd_x, (gain,)),
        (los_ref[1:2, :] * odd_y, (gain,)),
        (los_ref[0:1, :], thirds(-gain * cell_x)),
        (los_ref[1:2, :], thirds(-gain * cell_y)),
        (los_ref[2:3, :], thirds(gain * deep)[:2]),
    ):
        for a in thirds(one):
            for b in values:
                left.append(a)
                right.append(b)
    spare = feat.shape[1] - len(left)
    left.append(jnp.zeros((spare, npix), F32))
    right.append(jnp.zeros((spare, npatch), F32))
    feat[...] = jnp.concatenate(left, 0).T.astype(BF16)
    basis[...] = jnp.concatenate(right, 0).astype(BF16)
    prow[0:1, :] = cell_x
    for line in range(lines):
        away = (2 * (me * lines + line) + 1).astype(F32) - cell_y
        prow[1 + line : 2 + line, :] = away * away + deep * deep

    if chunks > 1:
        for i in range(loads):
            pltpu.make_async_copy(
                xs_ref.at[:, pl.ds(i * wide_load, wide_load)],
                stage.at[:, pl.ds(i * wide_load, wide_load)],
                r_in.at[i],
            ).wait()

            @pl.loop(0, per_load)
            def _(j):
                d = i * per_load + j
                for c in range(chunks):
                    at = pl.ds(pl.multiple_of(d * npix + c * span, span), span)
                    side_d = (d // many + half_me) % 2
                    xsend[c, d % many, side_d, :, :] = stage[:, at].astype(BF16)

    pl.semaphore_wait(barrier, n - 1)

    if chunks > 1:
        for c in range(chunks):

            @pl.loop(1, many)
            def _(k):
                to = (slot_me + k) % many
                pltpu.make_async_remote_copy(
                    src_ref=xsend.at[c, to],
                    dst_ref=got.at[c, slot_me],
                    send_sem=s_x,
                    recv_sem=r_x.at[c],
                    device_id=ident(half_me * many + to),
                    device_id_type=mesh_id,
                ).start()

        for c in range(chunks):
            got[c, slot_me, :, :, :] = xsend[c, slot_me, :, :, :]
    else:

        @pl.loop(1, n)
        def _(k):
            d = (me + k) % n
            pltpu.make_async_remote_copy(
                src_ref=xs_ref.at[d],
                dst_ref=got.at[0, me],
                send_sem=s_x,
                recv_sem=r_x.at[0],
                device_id=ident(d),
                device_id_type=mesh_id,
            ).start()

        own_copy = pltpu.make_async_copy(xs_ref.at[me], got.at[0, me], r_in.at[0])
        own_copy.start()

    rows = parts * n * ifg_dev
    nifg = n * ifg_dev
    ep = lax.broadcasted_iota(jnp.int32, (NEP, nifg), 0)
    later = (ep == pairs_ref[1:2, :]).astype(F32)
    earlier = (ep == pairs_ref[0:1, :]).astype(F32)
    design = (later - earlier).astype(BF16)
    slot = lax.broadcasted_iota(jnp.int32, (nifg, rows), 1)
    source = slot // (parts * ifg_dev) * ifg_dev + slot % ifg_dev
    spread = (lax.broadcasted_iota(jnp.int32, (nifg, rows), 0) == source).astype(F32).astype(BF16)
    design_half = jnp.dot(design, spread, preferred_element_type=F32).astype(BF16)
    sub = lax.broadcasted_iota(jnp.int32, (NEP, NEP), 0)
    lane = lax.broadcasted_iota(jnp.int32, (NEP, NEP), 1)
    normal = lax.dot_general(design, design, NT, preferred_element_type=F32)
    mat[...] = normal + jnp.where(sub == lane, damping, 0.0)

    def sweep(k):
        m = mat[...]
        col = jnp.sum(jnp.where(lane == k, m, 0.0), axis=1, keepdims=True)
        row = jnp.sum(jnp.where(sub == k, m, 0.0), axis=0, keepdims=True)
        wide_col = jnp.broadcast_to(col, (NEP, NEP))
        pivot = jnp.sum(jnp.where(sub == k, wide_col, 0.0), axis=0, keepdims=True)
        inv = 1.0 / pivot
        scaled = row * inv
        new = m - wide_col * scaled
        new = jnp.where(lane == k, wide_col * inv, new)
        new = jnp.where(sub == k, scaled, new)
        mat[...] = jnp.where((sub == k) & (lane == k), -inv, new)

    strip, wide = 128, 256
    per_line = IMG_W // strip
    turns = 2 * -(-NEP // (lines * per_line))
    swept = min(lines, NEP // (per_line * turns)) * per_line * turns

    slab = npatch // per_line

    def weigh(line):
        here = slice(line * IMG_W, (line + 1) * IMG_W)
        weight[...] = lax.dot_general(
            jnp.ones((EXTRA, LANES), F32),
            wacc[here, :],
            NT,
            precision=lax.Precision.HIGHEST,
            preferred_element_type=F32,
        ).astype(BF16)

    def gather_bound(line, t):
        here = slice(line * IMG_W, (line + 1) * IMG_W)
        cols = pl.ds(pl.multiple_of(t * slab, slab), slab)
        row = jnp.dot(weight[...], jnp.abs(green[here, cols]), preferred_element_type=F32)
        if line > 0:
            row = row + brow[:, cols]
        brow[:, cols] = row

    def generate(line):
        if line > 0:
            weigh(line - 1)

        @pl.loop(0, per_line)
        def _(t):
            if line > 0:
                gather_bound(line - 1, t)
            start = pl.multiple_of(line * IMG_W + t * strip, strip)
            mix = feat[pl.ds(start, strip), :]
            spot = t * strip + lax.broadcasted_iota(jnp.int32, (strip, LANES), 0)
            xpos = (2 * spot + 1).astype(F32)
            for q in range(turns):
                if (line + 1) * per_line * turns <= swept:
                    sweep((line * per_line + t) * turns + q)
            total = jnp.zeros((strip, LANES), F32)
            for c in range(npatch // wide):
                num = jnp.dot(
                    mix, basis[:, c * wide : (c + 1) * wide], preferred_element_type=F32
                )
                halves = []
                for j in range(wide // LANES):
                    at = slice(c * wide + j * LANES, c * wide + (j + 1) * LANES)
                    away = xpos - prow[0:1, at]
                    inv = lax.rsqrt(away * away + prow[1 + line : 2 + line, at])
                    g = num[:, j * LANES : (j + 1) * LANES] * (inv * inv * inv)
                    total = total + jnp.abs(g)
                    halves.append(g.astype(BF16))
                green[pl.ds(start, strip), c * wide : (c + 1) * wide] = jnp.concatenate(halves, 1)
            wacc[pl.ds(start, strip), :] = total

    def invert():
        @pl.loop(swept, NEP)
        def _(k):
            sweep(k)

        inverse = -mat[...]
        inv_hi = inverse.astype(BF16)
        rest = inverse - inv_hi.astype(F32)
        inv_mid = rest.astype(BF16)
        inv_lo = (rest - inv_mid.astype(F32)).astype(BF16)
        pseudo = (
            jnp.dot(inv_hi, design_half, preferred_element_type=F32)
            + jnp.dot(inv_mid, design_half, preferred_element_type=F32)
            + jnp.dot(inv_lo, design_half, preferred_element_type=F32)
        )
        which = (lax.broadcasted_iota(jnp.int32, (NEP, rows), 1) // ifg_dev) % parts
        if chunks > 1:
            cut = many * ifg_dev
            parted = [jnp.where(half_me == 0, pseudo[:, :cut], pseudo[:, cut:])]
        else:
            parted = [jnp.where(which == h, pseudo, 0.0) for h in range(parts)]
        result = []
        for keep in parted:
            hi = keep.astype(BF16)
            result.append((hi, (keep - hi.astype(F32)).astype(BF16)))
        return result

    def halve(c):
        settle(got.at[c], many - 1, r_x.at[c])
        ((hi, lo),) = pieces
        sums = []
        for part_of in range(2):
            stacked = got[c, :, part_of].reshape(many * ifg_dev, span)
            piece = jnp.dot(hi, stacked, preferred_element_type=F32)
            sums.append(piece + jnp.dot(lo, stacked, preferred_element_type=F32))
        over[c, :, :] = sums[1].astype(BF16)
        pltpu.make_async_remote_copy(
            src_ref=over.at[c],
            dst_ref=back.at[c],
            send_sem=s_m,
            recv_sem=r_m.at[c],
            device_id=ident(mirror),
            device_id_type=mesh_id,
        ).start()
        series[:, c * span : (c + 1) * span] = sums[0]

    ready = min(lines, -(-NEP // (per_line * turns)))
    halved = 0
    for line in range(lines):
        generate(line)
        if line == ready - 1:
            pieces = invert()
        if chunks > 1 and line >= ready - 1:
            upto = chunks if line == lines - 1 else min(line + 1, chunks)
            for c in range(halved, upto):
                halve(c)
            halved = upto

    block = 512
    weigh(lines - 1)

    @pl.loop(0, npatch // slab)
    def _(b):
        gather_bound(lines - 1, b)
        row = brow[:, pl.ds(pl.multiple_of(b * slab, slab), slab)]
        high = row.astype(BF16)
        low = (row - high.astype(F32)).astype(BF16)
        pick = lax.broadcasted_iota(jnp.int32, (EXTRA, slab), 0) == 0
        tail = jnp.where(pick, high.astype(F32), low.astype(F32)).astype(BF16)
        for j in range(slab // LANES):
            bsend[b * (slab // LANES) + j, :, :] = tail[:, j * LANES : (j + 1) * LANES]

    @pl.loop(1, n)
    def _(k):
        d = (me + k) % n
        pltpu.make_async_remote_copy(
            src_ref=bsend.at[d // reps],
            dst_ref=bpart.at[me],
            send_sem=s_b,
            recv_sem=r_b,
            device_id=ident(d),
            device_id_type=mesh_id,
        ).start()

    bpart[me, :, :] = bsend[mine, :, :]

    if chunks == 1:
        own_copy.wait()

    def solve(c):
        if chunks > 1:
            here = slice(c * span, (c + 1) * span)
            pltpu.make_async_copy(back.at[c], back.at[c], r_m.at[c]).wait()
            piece = series[:, here] + back[c].astype(F32)
            series[:, here] = piece
            resid[:, here] = piece.astype(BF16)
            return
        settle(got.at[0], n - 1, r_x.at[0])
        width = npix // parts
        stacked = got[0].reshape(rows, width)
        for h, (hi, lo) in enumerate(pieces):
            piece = jnp.dot(hi, stacked, preferred_element_type=F32)
            piece = piece + jnp.dot(lo, stacked, preferred_element_type=F32)
            series[:, h * width : (h + 1) * width] = piece
            resid[:, h * width : (h + 1) * width] = piece.astype(BF16)

    per_block = block // LANES
    blocks = npatch // block
    first_block = mine // per_block
    side = blocks // 2

    def place(b):
        return (first_block // side + 1 + b // side) % 2 * side + (first_block + 1 + b) % side

    for c in range(chunks - 1):
        solve(c)
        ks = slice(c * span, (c + 1) * span)

        @pl.loop(0, npatch // 1024)
        def _(b):
            cols = pl.ds(pl.multiple_of(b * 1024, 1024), 1024)
            out = jnp.dot(resid[:, ks], green[ks, cols], preferred_element_type=F32)
            if c > 0:
                out = out + guess[:, cols]
            guess[:, cols] = out

    solve(chunks - 1)

    def product(at, first):
        cols = pl.ds(pl.multiple_of(at * block, block), block)
        if first and chunks > 1:
            ks = slice((chunks - 1) * span, npix)
            out = jnp.dot(resid[:, ks], green[ks, cols], preferred_element_type=F32)
            return out + guess[:, cols]
        return jnp.dot(resid[...], green[:, cols], preferred_element_type=F32)

    def bounds():
        settle(bpart, n - 1, r_b)
        settle(bpart, n - 1, s_b)
        both = lax.fori_loop(
            1, n, lambda d, acc: acc + bpart[d].astype(F32), bpart[0].astype(F32)
        )
        return both[0:1] + both[1:2]

    def project(part, recv_sem, pair, pair_sem, first):
        @pl.loop(0, blocks)
        def _(b):
            at = place(b)
            half_out = product(at, first).astype(BF16)
            for j in range(per_block):
                send[at * per_block + j, :, :] = half_out[:, j * LANES : (j + 1) * LANES]
            for j in range(per_block):
                group = at * per_block + j
                for r in range(reps):
                    d = group * reps + r

                    @pl.when(d != me)
                    def _():
                        pltpu.make_async_remote_copy(
                            src_ref=send.at[group],
                            dst_ref=part.at[me],
                            send_sem=s_p,
                            recv_sem=recv_sem,
                            device_id=ident(d),
                            device_id_type=mesh_id,
                        ).start()

        part[me, :, :] = send[mine, :, :]
        settle(part, n - 1, recv_sem)
        settle(part, n - 1, s_p)
        bound = bounds() if first else None
        total = lax.fori_loop(
            1, n, lambda d, acc: acc + part[d].astype(F32), part[0].astype(F32)
        )
        return total, bound

    chips = n // 2
    per_pair = per_block // 2

    def project_split(part, recv_sem, pair, pair_sem, first):
        def forward(at):
            here = pl.ds(at * per_pair, per_pair)
            pltpu.make_async_copy(pair.at[here], pair.at[here], pair_sem.at[at]).wait()
            for j in range(per_pair):
                slot = at * per_pair + j
                send[slot, :, :] = (own[slot] + pair[slot].astype(F32)).astype(BF16)
            for j in range(per_pair):
                slot = at * per_pair + j

                @pl.when(slot != chip)
                def _():
                    pltpu.make_async_remote_copy(
                        src_ref=send.at[slot],
                        dst_ref=part.at[chip],
                        send_sem=s_p,
                        recv_sem=recv_sem,
                        device_id=ident(slot * 2 + core),
                        device_id_type=mesh_id,
                    ).start()

        @pl.loop(0, blocks)
        def _(b):
            at = place(b)
            out = product(at, first)
            for j in range(per_pair):
                even = out[:, 2 * j * LANES : (2 * j + 1) * LANES]
                odd = out[:, (2 * j + 1) * LANES : (2 * j + 2) * LANES]
                slot = at * per_pair + j
                own[slot, :, :] = jnp.where(core == 0, even, odd)
                half[slot, :, :] = jnp.where(core == 0, odd, even).astype(BF16)
            here = pl.ds(at * per_pair, per_pair)
            pltpu.make_async_remote_copy(
                src_ref=half.at[here],
                dst_ref=pair.at[here],
                send_sem=s_h,
                recv_sem=pair_sem.at[at],
                device_id=ident(partner),
                device_id_type=mesh_id,
            ).start()

            @pl.when(b > 0)
            def _():
                forward(place(b - 1))

        forward(place(blocks - 1))
        part[chip, :, :] = send[chip, :, :]
        settle(half, chips, s_h)
        bound = bounds() if first else None
        settle(part, chips - 1, recv_sem)
        settle(part, chips - 1, s_p)
        total = lax.fori_loop(
            1, chips, lambda d, acc: acc + part[d].astype(F32), part[0].astype(F32)
        )
        return total, bound

    tile = 512

    def share(slip, gath, recv_sem, pass_sem, target):
        gath[mine, :, :] = slip.astype(BF16)

        @pl.loop(1, gathered)
        def _(k):
            d = (me + (n - k * reps)) % n
            pltpu.make_async_remote_copy(
                src_ref=gath.at[mine],
                dst_ref=gath.at[mine],
                send_sem=s_g,
                recv_sem=recv_sem.at[first_block],
                device_id=ident(d),
                device_id_type=mesh_id,
            ).start()

        for i in range(blocks):
            at = (first_block + i) % blocks
            settle(gath, per_block - 1 if i == 0 else per_block, recv_sem.at[at])
            for j in range(per_block):
                full[:, j * LANES : (j + 1) * LANES] = gath[at * per_block + j]
            cols = pl.ds(pl.multiple_of(at * block, block), block)

            @pl.loop(0, npix // tile)
            def _(t):
                here = pl.ds(pl.multiple_of(t * tile, tile), tile)
                out = lax.dot_general(
                    full[:, 0:block], green[here, cols], NT, preferred_element_type=F32
                )
                if i > 0:
                    out = target[:, here] + out
                target[:, here] = out

        settle(gath, gathered - 1, s_g)

    each = chips // batches
    home = chip // each
    span_at = 2 * each * LANES

    def share_split(slip, gath, recv_sem, pass_sem, target):
        mine_at = core * chips + chip
        gath[mine_at, :, :] = slip.astype(BF16)

        def give(to, side_core):
            pltpu.make_async_remote_copy(
                src_ref=gath.at[mine_at],
                dst_ref=gath.at[mine_at],
                send_sem=s_g,
                recv_sem=recv_sem.at[home],
                device_id=ident(to * 2 + side_core),
                device_id_type=mesh_id,
            ).start()

        give(chip, 1 - core)
        for k in range(1, each):
            to = home * each + (chip + k) % each
            give(to, core)
            give(to, 1 - core)

        def order(i):
            if batches != 4:
                return (home + i) % batches
            low, high = i % 2, i // 2
            bit = home % 2
            near = bit + low - 2 * bit * low
            far = home // 2 + high - 2 * (home // 2) * high
            return 2 * far + near

        @pl.loop(1, batches)
        def _(i):
            for k in range(each):
                give(order(i) * each + (chip + k) % each, core)

        def passing(at):
            return pl.ds(core * chips + at * each, each)

        def collect(i):
            at = order(i)
            settle(gath, each, recv_sem.at[at])
            pltpu.make_async_remote_copy(
                src_ref=gath.at[passing(at)],
                dst_ref=gath.at[passing(at)],
                send_sem=s_f,
                recv_sem=pass_sem.at[at],
                device_id=ident(partner),
                device_id_type=mesh_id,
            ).start()

        target[:, 0:npix] = jnp.zeros((NEP, npix), F32)
        groups_in = 4
        rounds = npix // (1024 * groups_in)

        @pl.loop(0, batches)
        def _(i):
            at = order(i)

            @pl.when(i == 0)
            def _():
                settle(gath, 2 * each - 1, recv_sem.at[at])

            @pl.when(i > 0)
            def _():
                settle(gath, each, pass_sem.at[at])

            for j in range(each):
                for p in range(2):
                    lane = (2 * j + p) * LANES
                    full[:, lane : lane + LANES] = gath[p * chips + at * each + j]
            tall[...] = full[:, 0:span_at].T

            @pl.loop(0, rounds)
            def _(trip):
                @pl.when((i + 1 < batches) & (trip == rounds // 2))
                def _():
                    collect(i + 1)

                for sub_trip in range(groups_in):
                    start = (trip * groups_in + sub_trip) * 1024
                    flat = pl.ds(pl.multiple_of(start, 512), 512)
                    long = pl.ds(pl.multiple_of(start + 512, 512), 512)
                    wide_out = long_out = None
                    for k in range(0, span_at, 256):
                        ks = slice(k, k + 256)
                        cols = pl.ds(pl.multiple_of(at * span_at + k, 256), 256)
                        a = lax.dot_general(
                            full[:, ks], green[flat, cols], NT, preferred_element_type=F32
                        )
                        b = jnp.dot(green[long, cols], tall[ks, :], preferred_element_type=F32)
                        wide_out = a if wide_out is None else wide_out + a
                        long_out = b if long_out is None else long_out + b
                    target[:, flat] = target[:, flat] + wide_out
                    target[:, long] = target[:, long] + long_out.T

        settle(gath, 2 * each - 1 + (batches - 1) * each, s_g)
        settle(gath, (batches - 1) * each, s_f)

    if split:
        project, share = project_split, share_split
    sums, bound = project(part_a, r_pa, pair_a, r_ha, True)
    if chunks > 1:
        for c in range(chunks):
            settle(got.at[c], many - 1, s_x)
        settle(over, chunks, s_m)
    else:
        settle(got.at[0], n - 1, s_x)
    slip = sums / bound
    share(slip, gath_a, r_ga, r_fa, guess)
    resid[...] = (series[...] - guess[:, 0:npix]).astype(BF16)
    slip = slip + project(part_b, r_pb, pair_b, r_hb, False)[0] / bound
    slip_ref[...] = slip
    share(slip, gath_b, r_gb, r_fb, pred_ref)


def relay(pred_ref, slip_ref, pred_out, slip_out, pred_buf, slip_buf, sems):
    rows = 8
    count = pred_ref.shape[0] // rows
    moves = [(slip_ref, slip_buf, slip_out)]
    for i in range(count):
        at = pl.ds(i * rows, rows)
        moves.append((pred_ref.at[at], pred_buf.at[at], pred_out.at[at]))
    loads = [pltpu.make_async_copy(a, b, sems.at[0, i]) for i, (a, b, c) in enumerate(moves)]
    stores = [pltpu.make_async_copy(b, c, sems.at[1, i]) for i, (a, b, c) in enumerate(moves)]
    for load in loads:
        load.start()
    for load, store in zip(loads, stores):
        load.wait()
        store.start()
    for store in stores:
        store.wait()


def on_device(interferograms, epoch_pairs, los, patch_place, patch_depth):
    n = lax.axis_size(("pix", "rep"))
    me = lax.axis_index(("pix", "rep"))
    ifg_dev, total = interferograms.shape
    npix = total // n
    npatch = patch_depth.shape[0]
    own = npatch // n
    reps = max(LANES // own, 1)
    parts = max(16 // ifg_dev, 1)
    width = npix // parts
    lines = npix // IMG_W

    chunks = 1
    if ifg_dev % 8 == 0 and lines > 1:
        chunks, parts, width = lines, 1, IMG_W
        xs = interferograms
    else:
        xs = interferograms.astype(BF16).reshape(ifg_dev, n, parts, width)
        xs = xs.transpose(1, 2, 0, 3).reshape(n, parts * ifg_dev, width)
    inside = chunks > 1
    swap = (chunks, n // 2, 2, ifg_dev, width)
    groups = npatch // LANES
    cfg = (n, reps, npix, npatch, parts, ifg_dev, lines, chunks)
    chips = n // 2
    pairs = chips if reps == 1 else 1
    small = (1,) + (16, LANES)
    loads = 8 if n % 8 == 0 else 1
    batches = max(n // 8, 1)
    vmem = pl.BlockSpec(memory_space=pltpu.VMEM)
    piece = (NEP, LANES)
    block = 512
    dma = pltpu.SemaphoreType.DMA
    predicted, slip = pl.pallas_call(
        functools.partial(kernel, cfg),
        out_shape=(
            jax.ShapeDtypeStruct((NEP, npix), F32),
            jax.ShapeDtypeStruct((NEP, LANES), F32),
        ),
        in_specs=[vmem, vmem, vmem, vmem, pl.BlockSpec(memory_space=pl.ANY)],
        out_specs=(vmem, vmem),
        scratch_shapes=[
            pltpu.VMEM((npix, 32), BF16),
            pltpu.VMEM((32, npatch), BF16),
            pltpu.VMEM((1 + lines, npatch), F32),
            pltpu.VMEM((NEP, NEP), F32),
            pltpu.VMEM((npix, npatch), BF16),
            pltpu.VMEM((npix, LANES), F32),
            pltpu.VMEM((EXTRA, IMG_W), BF16),
            pltpu.VMEM((EXTRA, npatch), F32),
            pltpu.VMEM(swap if inside else (1, n, parts * ifg_dev, width), BF16),
            pltpu.VMEM((NEP, npix), F32),
            pltpu.VMEM((NEP, npix), BF16),
            pltpu.VMEM((groups, EXTRA, LANES), BF16),
            pltpu.VMEM((n, EXTRA, LANES), BF16),
            pltpu.VMEM((groups,) + piece, BF16),
            pltpu.VMEM((n,) + piece, BF16),
            pltpu.VMEM((n,) + piece, BF16),
            pltpu.VMEM((groups, NEP, LANES), BF16),
            pltpu.VMEM((groups, NEP, LANES), BF16),
            pltpu.VMEM((NEP, max(block, 2 * LANES * chips // batches)), BF16),
            pltpu.VMEM((2 * LANES * chips // batches, NEP), BF16),
            pltpu.VMEM((NEP, max(npix, npatch)), F32),
            pltpu.VMEM(interferograms.shape if inside else (8, LANES), F32),
            pltpu.VMEM(swap if inside else small, BF16),
            pltpu.VMEM((chunks, NEP, width) if inside else small, BF16),
            pltpu.VMEM((chunks, NEP, width) if inside else small, BF16),
            pltpu.VMEM((pairs,) + piece, F32),
            pltpu.VMEM((pairs,) + piece, BF16),
            pltpu.VMEM((pairs,) + piece, BF16),
            pltpu.VMEM((pairs,) + piece, BF16),
            dma,
            dma((chunks,)),
            dma((loads,)),
            dma,
            dma((chunks,)),
            dma,
            dma,
            dma,
            dma,
            dma,
            dma,
            dma((npatch // block,)),
            dma((npatch // block,)),
            dma,
            dma((max(npatch // block, batches),)),
            dma((max(npatch // block, batches),)),
            dma,
            dma((batches,)),
            dma((batches,)),
        ],
        compiler_params=pltpu.CompilerParams(
            collective_id=0, has_side_effects=True, vmem_limit_bytes=62 * 1024 * 1024
        ),
    )(epoch_pairs, los, patch_place, patch_depth[None], xs)
    anywhere = pl.BlockSpec(memory_space=pl.ANY)
    predicted, slip = pl.pallas_call(
        relay,
        out_shape=tuple(jax.ShapeDtypeStruct(a.shape, F32) for a in (predicted, slip)),
        in_specs=[anywhere, anywhere],
        out_specs=(anywhere, anywhere),
        scratch_shapes=[
            pltpu.VMEM(predicted.shape, F32),
            pltpu.VMEM(slip.shape, F32),
            dma((2, 1 + NEP // 8)),
        ],
    )(predicted, slip)
    if reps > 1:
        slip = lax.dynamic_slice_in_dim(slip, (me % reps) * own, own, 1)
    return (predicted, slip)


def solution(mesh):
    placed = (P(("pix", "rep"), None), P(), P(None, ("pix", "rep")), P(), P())
    return jax.shard_map(
        on_device,
        mesh=mesh,
        in_specs=placed,
        out_specs=(P(None, ("pix", "rep")), P(None, ("pix", "rep"))),
        check_vma=False,
    )
```

```python
import functools

import jax
import jax.numpy as jnp
from jax import lax
from jax.experimental import pallas as pl
from jax.experimental.pallas import tpu as pltpu
from jax.sharding import PartitionSpec as P

NEP = 64
IMG_W = 1024
LANES = 128

damping = 0.5

F32 = jnp.float32
BF16 = jnp.bfloat16
NT = (((1,), (1,)), ((), ()))
EXTRA = 16


def thirds(x):
    high = x.astype(BF16).astype(F32)
    rest = x - high
    mid = rest.astype(BF16).astype(F32)
    return high, mid, (rest - mid).astype(BF16).astype(F32)


def kernel(
    cfg,
    pairs_ref,
    los_ref,
    place_ref,
    depth_ref,
    xs_ref,
    pred_ref,
    slip_ref,
    feat,
    basis,
    prow,
    mat,
    green,
    wacc,
    weight,
    brow,
    got,
    series,
    resid,
    bsend,
    bpart,
    send,
    part_a,
    part_b,
    gath_a,
    gath_b,
    full,
    tall,
    guess,
    stage,
    xsend,
    over,
    back,
    own,
    half,
    pair_a,
    pair_b,
    s_x,
    r_x,
    r_in,
    s_m,
    r_m,
    s_b,
    r_b,
    s_p,
    r_pa,
    r_pb,
    s_h,
    r_ha,
    r_hb,
    s_g,
    r_ga,
    r_gb,
    s_f,
    r_fa,
    r_fb,
):
    n, reps, npix, npatch, parts, ifg_dev, lines, chunks = cfg
    me = lax.axis_index(("pix", "rep"))
    rep_size = lax.axis_size("rep")
    groups = npatch // LANES
    mine = me // reps
    gathered = n // reps
    split = reps == 1 and n % 8 == 0
    core = me % 2
    chip = me // 2
    partner = me + 1 - 2 * core
    batches = n // 8
    many = n // 2
    slot_me = me % many
    half_me = me // many
    mirror = (me + many) % n
    mesh_id = pl.DeviceIdType.MESH

    def ident(d):
        return {"pix": d // rep_size, "rep": d % rep_size}

    def settle(buf, count, sem):
        view = buf.at[pl.ds(0, count)]
        pltpu.make_async_copy(view, view, sem).wait()

    barrier = pltpu.get_barrier_semaphore()

    @pl.loop(1, n)
    def _(k):
        pl.semaphore_signal(
            barrier, inc=1, device_id=ident((me + k) % n), device_id_type=mesh_id
        )

    if chunks > 1:
        loads = r_in.shape[0]
        per_load = n // loads
        wide_load = per_load * npix
        span = npix // chunks
        for i in range(loads):
            pltpu.make_async_copy(
                xs_ref.at[:, pl.ds(i * wide_load, wide_load)],
                stage.at[:, pl.ds(i * wide_load, wide_load)],
                r_in.at[i],
            ).start()

    pixel = lax.broadcasted_iota(jnp.int32, (1, npix), 1)
    odd_x = (2 * (pixel % IMG_W) + 1).astype(F32)
    odd_y = (2 * (me * lines + pixel // IMG_W) + 1).astype(F32)
    cell_x = (8 * place_ref[0:1, :] + 4).astype(F32)
    cell_y = (8 * place_ref[1:2, :] + 4).astype(F32)
    deep = (10 + 5 * depth_ref[...]).astype(F32)
    gain = 20.0 * deep
    left, right = [], []
    for one, values in (
        (los_ref[0:1, :] * odd_x, (gain,)),
        (los_ref[1:2, :] * odd_y, (gain,)),
        (los_ref[0:1, :], thirds(-gain * cell_x)),
        (los_ref[1:2, :], thirds(-gain * cell_y)),
        (los_ref[2:3, :], thirds(gain * deep)[:2]),
    ):
        for a in thirds(one):
            for b in values:
                left.append(a)
                right.append(b)
    spare = feat.shape[1] - len(left)
    left.append(jnp.zeros((spare, npix), F32))
    right.append(jnp.zeros((spare, npatch), F32))
    feat[...] = jnp.concatenate(left, 0).T.astype(BF16)
    basis[...] = jnp.concatenate(right, 0).astype(BF16)
    prow[0:1, :] = cell_x
    for line in range(lines):
        away = (2 * (me * lines + line) + 1).astype(F32) - cell_y
        prow[1 + line : 2 + line, :] = away * away + deep * deep

    if chunks > 1:
        for i in range(loads):
            pltpu.make_async_copy(
                xs_ref.at[:, pl.ds(i * wide_load, wide_load)],
                stage.at[:, pl.ds(i * wide_load, wide_load)],
                r_in.at[i],
            ).wait()

            @pl.loop(0, per_load)
            def _(j):
                d = i * per_load + j
                for c in range(chunks):
                    at = pl.ds(pl.multiple_of(d * npix + c * span, span), span)
                    side_d = (d // many + half_me) % 2
                    xsend[c, d % many, side_d, :, :] = stage[:, at].astype(BF16)

    pl.semaphore_wait(barrier, n - 1)

    if chunks > 1:
        for c in range(chunks):

            @pl.loop(1, many)
            def _(k):
                to = (slot_me + k) % many
                pltpu.make_async_remote_copy(
                    src_ref=xsend.at[c, to],
                    dst_ref=got.at[c, slot_me],
                    send_sem=s_x,
                    recv_sem=r_x.at[c],
                    device_id=ident(half_me * many + to),
                    device_id_type=mesh_id,
                ).start()

        for c in range(chunks):
            got[c, slot_me, :, :, :] = xsend[c, slot_me, :, :, :]
    else:

        @pl.loop(1, n)
        def _(k):
            d = (me + k) % n
            pltpu.make_async_remote_copy(
                src_ref=xs_ref.at[d],
                dst_ref=got.at[0, me],
                send_sem=s_x,
                recv_sem=r_x.at[0],
                device_id=ident(d),
                device_id_type=mesh_id,
            ).start()

        own_copy = pltpu.make_async_copy(xs_ref.at[me], got.at[0, me], r_in.at[0])
        own_copy.start()

    rows = parts * n * ifg_dev
    nifg = n * ifg_dev
    ep = lax.broadcasted_iota(jnp.int32, (NEP, nifg), 0)
    later = (ep == pairs_ref[1:2, :]).astype(F32)
    earlier = (ep == pairs_ref[0:1, :]).astype(F32)
    design = (later - earlier).astype(BF16)
    slot = lax.broadcasted_iota(jnp.int32, (nifg, rows), 1)
    source = slot // (parts * ifg_dev) * ifg_dev + slot % ifg_dev
    spread = (lax.broadcasted_iota(jnp.int32, (nifg, rows), 0) == source).astype(F32).astype(BF16)
    design_half = jnp.dot(design, spread, preferred_element_type=F32).astype(BF16)
    sub = lax.broadcasted_iota(jnp.int32, (NEP, NEP), 0)
    lane = lax.broadcasted_iota(jnp.int32, (NEP, NEP), 1)
    normal = lax.dot_general(design, design, NT, preferred_element_type=F32)
    mat[...] = normal + jnp.where(sub == lane, damping, 0.0)

    def sweep(k):
        m = mat[...]
        col = jnp.sum(jnp.where(lane == k, m, 0.0), axis=1, keepdims=True)
        row = jnp.sum(jnp.where(sub == k, m, 0.0), axis=0, keepdims=True)
        wide_col = jnp.broadcast_to(col, (NEP, NEP))
        pivot = jnp.sum(jnp.where(sub == k, wide_col, 0.0), axis=0, keepdims=True)
        inv = 1.0 / pivot
        scaled = row * inv
        new = m - wide_col * scaled
        new = jnp.where(lane == k, wide_col * inv, new)
        new = jnp.where(sub == k, scaled, new)
        mat[...] = jnp.where((sub == k) & (lane == k), -inv, new)

    strip, wide = 128, 256
    per_line = IMG_W // strip
    turns = 2 * -(-NEP // (lines * per_line))
    swept = min(lines, NEP // (per_line * turns)) * per_line * turns

    slab = npatch // per_line

    def weigh(line):
        here = slice(line * IMG_W, (line + 1) * IMG_W)
        weight[...] = lax.dot_general(
            jnp.ones((EXTRA, LANES), F32),
            wacc[here, :],
            NT,
            precision=lax.Precision.HIGHEST,
            preferred_element_type=F32,
        ).astype(BF16)

    def gather_bound(line, t):
        here = slice(line * IMG_W, (line + 1) * IMG_W)
        cols = pl.ds(pl.multiple_of(t * slab, slab), slab)
        row = jnp.dot(weight[...], jnp.abs(green[here, cols]), preferred_element_type=F32)
        if line > 0:
            row = row + brow[:, cols]
        brow[:, cols] = row

    def generate(line):
        if line > 0:
            weigh(line - 1)

        @pl.loop(0, per_line)
        def _(t):
            if line > 0:
                gather_bound(line - 1, t)
            start = pl.multiple_of(line * IMG_W + t * strip, strip)
            mix = feat[pl.ds(start, strip), :]
            spot = t * strip + lax.broadcasted_iota(jnp.int32, (strip, LANES), 0)
            xpos = (2 * spot + 1).astype(F32)
            for q in range(turns):
                if (line + 1) * per_line * turns <= swept:
                    sweep((line * per_line + t) * turns + q)
            total = jnp.zeros((strip, LANES), F32)
            for c in range(npatch // wide):
                num = jnp.dot(
                    mix, basis[:, c * wide : (c + 1) * wide], preferred_element_type=F32
                )
                halves = []
                for j in range(wide // LANES):
                    at = slice(c * wide + j * LANES, c * wide + (j + 1) * LANES)
                    away = xpos - prow[0:1, at]
                    inv = lax.rsqrt(away * away + prow[1 + line : 2 + line, at])
                    g = num[:, j * LANES : (j + 1) * LANES] * (inv * inv * inv)
                    total = total + jnp.abs(g)
                    halves.append(g.astype(BF16))
                green[pl.ds(start, strip), c * wide : (c + 1) * wide] = jnp.concatenate(halves, 1)
            wacc[pl.ds(start, strip), :] = total

    def invert():
        @pl.loop(swept, NEP)
        def _(k):
            sweep(k)

        inverse = -mat[...]
        inv_hi = inverse.astype(BF16)
        rest = inverse - inv_hi.astype(F32)
        inv_mid = rest.astype(BF16)
        inv_lo = (rest - inv_mid.astype(F32)).astype(BF16)
        pseudo = (
            jnp.dot(inv_hi, design_half, preferred_element_type=F32)
            + jnp.dot(inv_mid, design_half, preferred_element_type=F32)
            + jnp.dot(inv_lo, design_half, preferred_element_type=F32)
        )
        which = (lax.broadcasted_iota(jnp.int32, (NEP, rows), 1) // ifg_dev) % parts
        if chunks > 1:
            cut = many * ifg_dev
            parted = [jnp.where(half_me == 0, pseudo[:, :cut], pseudo[:, cut:])]
        else:
            parted = [jnp.where(which == h, pseudo, 0.0) for h in range(parts)]
        result = []
        for keep in parted:
            hi = keep.astype(BF16)
            result.append((hi, (keep - hi.astype(F32)).astype(BF16)))
        return result

    def halve(c):
        settle(got.at[c], many - 1, r_x.at[c])
        ((hi, lo),) = pieces
        sums = []
        for part_of in range(2):
            stacked = got[c, :, part_of].reshape(many * ifg_dev, span)
            piece = jnp.dot(hi, stacked, preferred_element_type=F32)
            sums.append(piece + jnp.dot(lo, stacked, preferred_element_type=F32))
        over[c, :, :] = sums[1].astype(BF16)
        pltpu.make_async_remote_copy(
            src_ref=over.at[c],
            dst_ref=back.at[c],
            send_sem=s_m,
            recv_sem=r_m.at[c],
            device_id=ident(mirror),
            device_id_type=mesh_id,
        ).start()
        series[:, c * span : (c + 1) * span] = sums[0]

    ready = min(lines, -(-NEP // (per_line * turns)))
    halved = 0
    for line in range(lines):
        generate(line)
        if line == ready - 1:
            pieces = invert()
        if chunks > 1 and line >= ready - 1:
            upto = chunks if line == lines - 1 else min(line + 1, chunks)
            for c in range(halved, upto):
                halve(c)
            halved = upto

    block = 512
    weigh(lines - 1)

    @pl.loop(0, npatch // slab)
    def _(b):
        gather_bound(lines - 1, b)
        row = brow[:, pl.ds(pl.multiple_of(b * slab, slab), slab)]
        high = row.astype(BF16)
        low = (row - high.astype(F32)).astype(BF16)
        pick = lax.broadcasted_iota(jnp.int32, (EXTRA, slab), 0) == 0
        tail = jnp.where(pick, high.astype(F32), low.astype(F32)).astype(BF16)
        for j in range(slab // LANES):
            bsend[b * (slab // LANES) + j, :, :] = tail[:, j * LANES : (j + 1) * LANES]

    @pl.loop(1, n)
    def _(k):
        d = (me + k) % n
        pltpu.make_async_remote_copy(
            src_ref=bsend.at[d // reps],
            dst_ref=bpart.at[me],
            send_sem=s_b,
            recv_sem=r_b,
            device_id=ident(d),
            device_id_type=mesh_id,
        ).start()

    bpart[me, :, :] = bsend[mine, :, :]

    if chunks == 1:
        own_copy.wait()

    def solve(c):
        if chunks > 1:
            here = slice(c * span, (c + 1) * span)
            pltpu.make_async_copy(back.at[c], back.at[c], r_m.at[c]).wait()
            piece = series[:, here] + back[c].astype(F32)
            series[:, here] = piece
            resid[:, here] = piece.astype(BF16)
            return
        settle(got.at[0], n - 1, r_x.at[0])
        width = npix // parts
        stacked = got[0].reshape(rows, width)
        for h, (hi, lo) in enumerate(pieces):
            piece = jnp.dot(hi, stacked, preferred_element_type=F32)
            piece = piece + jnp.dot(lo, stacked, preferred_element_type=F32)
            series[:, h * width : (h + 1) * width] = piece
            resid[:, h * width : (h + 1) * width] = piece.astype(BF16)

    per_block = block // LANES
    blocks = npatch // block
    first_block = mine // per_block
    side = blocks // 2

    def place(b):
        return (first_block // side + 1 + b // side) % 2 * side + (first_block + 1 + b) % side

    for c in range(chunks - 1):
        solve(c)
        ks = slice(c * span, (c + 1) * span)

        @pl.loop(0, npatch // 1024)
        def _(b):
            cols = pl.ds(pl.multiple_of(b * 1024, 1024), 1024)
            out = jnp.dot(resid[:, ks], green[ks, cols], preferred_element_type=F32)
            if c > 0:
                out = out + guess[:, cols]
            guess[:, cols] = out

    solve(chunks - 1)

    def product(at, first):
        cols = pl.ds(pl.multiple_of(at * block, block), block)
        if first and chunks > 1:
            ks = slice((chunks - 1) * span, npix)
            out = jnp.dot(resid[:, ks], green[ks, cols], preferred_element_type=F32)
            return out + guess[:, cols]
        return jnp.dot(resid[...], green[:, cols], preferred_element_type=F32)

    def bounds():
        settle(bpart, n - 1, r_b)
        settle(bpart, n - 1, s_b)
        both = lax.fori_loop(
            1, n, lambda d, acc: acc + bpart[d].astype(F32), bpart[0].astype(F32)
        )
        return both[0:1] + both[1:2]

    def project(part, recv_sem, pair, pair_sem, first):
        @pl.loop(0, blocks)
        def _(b):
            at = place(b)
            half_out = product(at, first).astype(BF16)
            for j in range(per_block):
                send[at * per_block + j, :, :] = half_out[:, j * LANES : (j + 1) * LANES]
            for j in range(per_block):
                group = at * per_block + j
                for r in range(reps):
                    d = group * reps + r

                    @pl.when(d != me)
                    def _():
                        pltpu.make_async_remote_copy(
                            src_ref=send.at[group],
                            dst_ref=part.at[me],
                            send_sem=s_p,
                            recv_sem=recv_sem,
                            device_id=ident(d),
                            device_id_type=mesh_id,
                        ).start()

        part[me, :, :] = send[mine, :, :]
        settle(part, n - 1, recv_sem)
        settle(part, n - 1, s_p)
        bound = bounds() if first else None
        total = lax.fori_loop(
            1, n, lambda d, acc: acc + part[d].astype(F32), part[0].astype(F32)
        )
        return total, bound

    chips = n // 2
    per_pair = per_block // 2

    def project_split(part, recv_sem, pair, pair_sem, first):
        def forward(at):
            here = pl.ds(at * per_pair, per_pair)
            pltpu.make_async_copy(pair.at[here], pair.at[here], pair_sem.at[at]).wait()
            for j in range(per_pair):
                slot = at * per_pair + j
                send[slot, :, :] = (own[slot] + pair[slot].astype(F32)).astype(BF16)
            for j in range(per_pair):
                slot = at * per_pair + j

                @pl.when(slot != chip)
                def _():
                    pltpu.make_async_remote_copy(
                        src_ref=send.at[slot],
                        dst_ref=part.at[chip],
                        send_sem=s_p,
                        recv_sem=recv_sem,
                        device_id=ident(slot * 2 + core),
                        device_id_type=mesh_id,
                    ).start()

        @pl.loop(0, blocks)
        def _(b):
            at = place(b)
            out = product(at, first)
            for j in range(per_pair):
                even = out[:, 2 * j * LANES : (2 * j + 1) * LANES]
                odd = out[:, (2 * j + 1) * LANES : (2 * j + 2) * LANES]
                slot = at * per_pair + j
                own[slot, :, :] = jnp.where(core == 0, even, odd)
                half[slot, :, :] = jnp.where(core == 0, odd, even).astype(BF16)
            here = pl.ds(at * per_pair, per_pair)
            pltpu.make_async_remote_copy(
                src_ref=half.at[here],
                dst_ref=pair.at[here],
                send_sem=s_h,
                recv_sem=pair_sem.at[at],
                device_id=ident(partner),
                device_id_type=mesh_id,
            ).start()

            @pl.when(b > 0)
            def _():
                forward(place(b - 1))

        forward(place(blocks - 1))
        part[chip, :, :] = send[chip, :, :]
        settle(half, chips, s_h)
        bound = bounds() if first else None
        settle(part, chips - 1, recv_sem)
        settle(part, chips - 1, s_p)
        total = lax.fori_loop(
            1, chips, lambda d, acc: acc + part[d].astype(F32), part[0].astype(F32)
        )
        return total, bound

    tile = 512

    def share(slip, gath, recv_sem, pass_sem, target):
        gath[mine, :, :] = slip.astype(BF16)

        @pl.loop(1, gathered)
        def _(k):
            d = (me + (n - k * reps)) % n
            pltpu.make_async_remote_copy(
                src_ref=gath.at[mine],
                dst_ref=gath.at[mine],
                send_sem=s_g,
                recv_sem=recv_sem.at[first_block],
                device_id=ident(d),
                device_id_type=mesh_id,
            ).start()

        for i in range(blocks):
            at = (first_block + i) % blocks
            settle(gath, per_block - 1 if i == 0 else per_block, recv_sem.at[at])
            for j in range(per_block):
                full[:, j * LANES : (j + 1) * LANES] = gath[at * per_block + j]
            cols = pl.ds(pl.multiple_of(at * block, block), block)

            @pl.loop(0, npix // tile)
            def _(t):
                here = pl.ds(pl.multiple_of(t * tile, tile), tile)
                out = lax.dot_general(
                    full[:, 0:block], green[here, cols], NT, preferred_element_type=F32
                )
                if i > 0:
                    out = target[:, here] + out
                target[:, here] = out

        settle(gath, gathered - 1, s_g)

    each = chips // batches
    home = chip // each
    span_at = 2 * each * LANES

    def share_split(slip, gath, recv_sem, pass_sem, target):
        mine_at = core * chips + chip
        gath[mine_at, :, :] = slip.astype(BF16)

        def give(to, side_core):
            pltpu.make_async_remote_copy(
                src_ref=gath.at[mine_at],
                dst_ref=gath.at[mine_at],
                send_sem=s_g,
                recv_sem=recv_sem.at[home],
                device_id=ident(to * 2 + side_core),
                device_id_type=mesh_id,
            ).start()

        give(chip, 1 - core)
        for k in range(1, each):
            to = home * each + (chip + k) % each
            give(to, core)
            give(to, 1 - core)

        def order(i):
            if batches != 4:
                return (home + i) % batches
            low, high = i % 2, i // 2
            bit = home % 2
            near = bit + low - 2 * bit * low
            far = home // 2 + high - 2 * (home // 2) * high
            return 2 * far + near

        @pl.loop(1, batches)
        def _(i):
            for k in range(each):
                give(order(i) * each + (chip + k) % each, core)

        def passing(at):
            return pl.ds(core * chips + at * each, each)

        def collect(i):
            at = order(i)
            settle(gath, each, recv_sem.at[at])
            pltpu.make_async_remote_copy(
                src_ref=gath.at[passing(at)],
                dst_ref=gath.at[passing(at)],
                send_sem=s_f,
                recv_sem=pass_sem.at[at],
                device_id=ident(partner),
                device_id_type=mesh_id,
            ).start()

        target[:, 0:npix] = jnp.zeros((NEP, npix), F32)

        @pl.loop(0, batches)
        def _(i):
            at = order(i)

            @pl.when(i == 0)
            def _():
                settle(gath, 2 * each - 1, recv_sem.at[at])

            @pl.when(i > 0)
            def _():
                settle(gath, each, pass_sem.at[at])

            for j in range(each):
                for p in range(2):
                    lane = (2 * j + p) * LANES
                    full[:, lane : lane + LANES] = gath[p * chips + at * each + j]
            tall[...] = full[:, 0:span_at].T

            @pl.when(i + 1 < batches)
            def _():
                collect(i + 1)

            for start in range(0, npix, 1024):
                flat = slice(start, start + 512)
                long = slice(start + 512, start + 1024)
                wide_out = long_out = None
                for k in range(0, span_at, 256):
                    ks = slice(k, k + 256)
                    cols = pl.ds(pl.multiple_of(at * span_at + k, 256), 256)
                    a = lax.dot_general(
                        full[:, ks], green[flat, cols], NT, preferred_element_type=F32
                    )
                    b = jnp.dot(green[long, cols], tall[ks, :], preferred_element_type=F32)
                    wide_out = a if wide_out is None else wide_out + a
                    long_out = b if long_out is None else long_out + b
                target[:, flat] = target[:, flat] + wide_out
                target[:, long] = target[:, long] + long_out.T

        settle(gath, 2 * each - 1 + (batches - 1) * each, s_g)
        settle(gath, (batches - 1) * each, s_f)

    if split:
        project, share = project_split, share_split
    sums, bound = project(part_a, r_pa, pair_a, r_ha, True)
    if chunks > 1:
        for c in range(chunks):
            settle(got.at[c], many - 1, s_x)
        settle(over, chunks, s_m)
    else:
        settle(got.at[0], n - 1, s_x)
    slip = sums / bound
    share(slip, gath_a, r_ga, r_fa, guess)
    resid[...] = (series[...] - guess[:, 0:npix]).astype(BF16)
    slip = slip + project(part_b, r_pb, pair_b, r_hb, False)[0] / bound
    slip_ref[...] = slip
    share(slip, gath_b, r_gb, r_fb, pred_ref)


def on_device(interferograms, epoch_pairs, los, patch_place, patch_depth):
    n = lax.axis_size(("pix", "rep"))
    me = lax.axis_index(("pix", "rep"))
    ifg_dev, total = interferograms.shape
    npix = total // n
    npatch = patch_depth.shape[0]
    own = npatch // n
    reps = max(LANES // own, 1)
    parts = max(16 // ifg_dev, 1)
    width = npix // parts
    lines = npix // IMG_W

    chunks = 1
    if ifg_dev % 8 == 0 and lines > 1:
        chunks, parts, width = lines, 1, IMG_W
        xs = interferograms
    else:
        xs = interferograms.astype(BF16).reshape(ifg_dev, n, parts, width)
        xs = xs.transpose(1, 2, 0, 3).reshape(n, parts * ifg_dev, width)
    inside = chunks > 1
    swap = (chunks, n // 2, 2, ifg_dev, width)
    groups = npatch // LANES
    cfg = (n, reps, npix, npatch, parts, ifg_dev, lines, chunks)
    chips = n // 2
    pairs = chips if reps == 1 else 1
    small = (1,) + (16, LANES)
    loads = 8 if n % 8 == 0 else 1
    batches = max(n // 8, 1)
    vmem = pl.BlockSpec(memory_space=pltpu.VMEM)
    piece = (NEP, LANES)
    block = 512
    dma = pltpu.SemaphoreType.DMA
    predicted, slip = pl.pallas_call(
        functools.partial(kernel, cfg),
        out_shape=(
            pltpu.VMEM((NEP, npix), F32),
            pltpu.VMEM((NEP, LANES), F32),
        ),
        in_specs=[vmem, vmem, vmem, vmem, pl.BlockSpec(memory_space=pl.ANY)],
        out_specs=(vmem, vmem),
        scratch_shapes=[
            pltpu.VMEM((npix, 32), BF16),
            pltpu.VMEM((32, npatch), BF16),
            pltpu.VMEM((1 + lines, npatch), F32),
            pltpu.VMEM((NEP, NEP), F32),
            pltpu.VMEM((npix, npatch), BF16),
            pltpu.VMEM((npix, LANES), F32),
            pltpu.VMEM((EXTRA, IMG_W), BF16),
            pltpu.VMEM((EXTRA, npatch), F32),
            pltpu.VMEM(swap if inside else (1, n, parts * ifg_dev, width), BF16),
            pltpu.VMEM((NEP, npix), F32),
            pltpu.VMEM((NEP, npix), BF16),
            pltpu.VMEM((groups, EXTRA, LANES), BF16),
            pltpu.VMEM((n, EXTRA, LANES), BF16),
            pltpu.VMEM((groups,) + piece, BF16),
            pltpu.VMEM((n,) + piece, BF16),
            pltpu.VMEM((n,) + piece, BF16),
            pltpu.VMEM((groups, NEP, LANES), BF16),
            pltpu.VMEM((groups, NEP, LANES), BF16),
            pltpu.VMEM((NEP, max(block, 2 * LANES * chips // batches)), BF16),
            pltpu.VMEM((2 * LANES * chips // batches, NEP), BF16),
            pltpu.VMEM((NEP, max(npix, npatch)), F32),
            pltpu.VMEM(interferograms.shape if inside else (8, LANES), F32),
            pltpu.VMEM(swap if inside else small, BF16),
            pltpu.VMEM((chunks, NEP, width) if inside else small, BF16),
            pltpu.VMEM((chunks, NEP, width) if inside else small, BF16),
            pltpu.VMEM((pairs,) + piece, F32),
            pltpu.VMEM((pairs,) + piece, BF16),
            pltpu.VMEM((pairs,) + piece, BF16),
            pltpu.VMEM((pairs,) + piece, BF16),
            dma,
            dma((chunks,)),
            dma((loads,)),
            dma,
            dma((chunks,)),
            dma,
            dma,
            dma,
            dma,
            dma,
            dma,
            dma((npatch // block,)),
            dma((npatch // block,)),
            dma,
            dma((max(npatch // block, batches),)),
            dma((max(npatch // block, batches),)),
            dma,
            dma((batches,)),
            dma((batches,)),
        ],
        compiler_params=pltpu.CompilerParams(
            collective_id=0, has_side_effects=True, vmem_limit_bytes=59 * 1024 * 1024
        ),
    )(epoch_pairs, los, patch_place, patch_depth[None], xs)
    if reps > 1:
        slip = lax.dynamic_slice_in_dim(slip, (me % reps) * own, own, 1)
    return (predicted, slip)


def solution(mesh):
    placed = (P(("pix", "rep"), None), P(), P(None, ("pix", "rep")), P(), P())
    return jax.shard_map(
        on_device,
        mesh=mesh,
        in_specs=placed,
        out_specs=(P(None, ("pix", "rep")), P(None, ("pix", "rep"))),
        check_vma=False,
    )
```

```python
import functools

import jax
import jax.numpy as jnp
from jax import lax
from jax.experimental import pallas as pl
from jax.experimental.pallas import tpu as pltpu
from jax.sharding import PartitionSpec as P

NEP = 64
IMG_W = 1024
LANES = 128

damping = 0.5

F32 = jnp.float32
BF16 = jnp.bfloat16
NT = (((1,), (1,)), ((), ()))
EXTRA = 16


def thirds(x):
    high = x.astype(BF16).astype(F32)
    rest = x - high
    mid = rest.astype(BF16).astype(F32)
    return high, mid, (rest - mid).astype(BF16).astype(F32)


def kernel(
    cfg,
    pairs_ref,
    los_ref,
    place_ref,
    depth_ref,
    xs_ref,
    pred_ref,
    slip_ref,
    feat,
    basis,
    prow,
    mat,
    green,
    wacc,
    weight,
    brow,
    got,
    series,
    resid,
    bsend,
    bpart,
    send,
    part_a,
    part_b,
    gath_a,
    gath_b,
    full,
    tall,
    guess,
    stage,
    xsend,
    over,
    back,
    own,
    half,
    pair_a,
    pair_b,
    s_x,
    r_x,
    r_in,
    s_m,
    r_m,
    s_b,
    r_b,
    s_p,
    r_pa,
    r_pb,
    s_h,
    r_ha,
    r_hb,
    s_g,
    r_ga,
    r_gb,
    s_f,
    r_fa,
    r_fb,
):
    n, reps, npix, npatch, parts, ifg_dev, lines, chunks = cfg
    me = lax.axis_index(("pix", "rep"))
    rep_size = lax.axis_size("rep")
    groups = npatch // LANES
    mine = me // reps
    gathered = n // reps
    split = reps == 1 and n % 8 == 0
    core = me % 2
    chip = me // 2
    partner = me + 1 - 2 * core
    batches = n // 8
    many = n // 2
    slot_me = me % many
    half_me = me // many
    mirror = (me + many) % n
    mesh_id = pl.DeviceIdType.MESH

    def ident(d):
        return {"pix": d // rep_size, "rep": d % rep_size}

    def settle(buf, count, sem):
        view = buf.at[pl.ds(0, count)]
        pltpu.make_async_copy(view, view, sem).wait()

    barrier = pltpu.get_barrier_semaphore()

    @pl.loop(1, n)
    def _(k):
        pl.semaphore_signal(
            barrier, inc=1, device_id=ident((me + k) % n), device_id_type=mesh_id
        )

    if chunks > 1:
        loads = r_in.shape[0]
        per_load = n // loads
        wide_load = per_load * npix
        span = npix // chunks
        for i in range(loads):
            pltpu.make_async_copy(
                xs_ref.at[:, pl.ds(i * wide_load, wide_load)],
                stage.at[:, pl.ds(i * wide_load, wide_load)],
                r_in.at[i],
            ).start()

    pixel = lax.broadcasted_iota(jnp.int32, (1, npix), 1)
    odd_x = (2 * (pixel % IMG_W) + 1).astype(F32)
    odd_y = (2 * (me * lines + pixel // IMG_W) + 1).astype(F32)
    cell_x = (8 * place_ref[0:1, :] + 4).astype(F32)
    cell_y = (8 * place_ref[1:2, :] + 4).astype(F32)
    deep = (10 + 5 * depth_ref[...]).astype(F32)
    gain = 20.0 * deep
    left, right = [], []
    for one, values in (
        (los_ref[0:1, :] * odd_x, (gain,)),
        (los_ref[1:2, :] * odd_y, (gain,)),
        (los_ref[0:1, :], thirds(-gain * cell_x)),
        (los_ref[1:2, :], thirds(-gain * cell_y)),
        (los_ref[2:3, :], thirds(gain * deep)[:2]),
    ):
        for a in thirds(one):
            for b in values:
                left.append(a)
                right.append(b)
    spare = feat.shape[1] - len(left)
    left.append(jnp.zeros((spare, npix), F32))
    right.append(jnp.zeros((spare, npatch), F32))
    feat[...] = jnp.concatenate(left, 0).T.astype(BF16)
    basis[...] = jnp.concatenate(right, 0).astype(BF16)
    prow[0:1, :] = cell_x
    for line in range(lines):
        away = (2 * (me * lines + line) + 1).astype(F32) - cell_y
        prow[1 + line : 2 + line, :] = away * away + deep * deep

    if chunks > 1:
        for i in range(loads):
            pltpu.make_async_copy(
                xs_ref.at[:, pl.ds(i * wide_load, wide_load)],
                stage.at[:, pl.ds(i * wide_load, wide_load)],
                r_in.at[i],
            ).wait()

            @pl.loop(0, per_load)
            def _(j):
                d = i * per_load + j
                for c in range(chunks):
                    at = pl.ds(pl.multiple_of(d * npix + c * span, span), span)
                    side_d = (d // many + half_me) % 2
                    xsend[c, d % many, side_d, :, :] = stage[:, at].astype(BF16)

    pl.semaphore_wait(barrier, n - 1)

    if chunks > 1:
        for c in range(chunks):

            @pl.loop(1, many)
            def _(k):
                to = (slot_me + k) % many
                pltpu.make_async_remote_copy(
                    src_ref=xsend.at[c, to],
                    dst_ref=got.at[c, slot_me],
                    send_sem=s_x,
                    recv_sem=r_x.at[c],
                    device_id=ident(half_me * many + to),
                    device_id_type=mesh_id,
                ).start()

        for c in range(chunks):
            got[c, slot_me, :, :, :] = xsend[c, slot_me, :, :, :]
    else:

        @pl.loop(1, n)
        def _(k):
            d = (me + k) % n
            pltpu.make_async_remote_copy(
                src_ref=xs_ref.at[d],
                dst_ref=got.at[0, me],
                send_sem=s_x,
                recv_sem=r_x.at[0],
                device_id=ident(d),
                device_id_type=mesh_id,
            ).start()

        own_copy = pltpu.make_async_copy(xs_ref.at[me], got.at[0, me], r_in.at[0])
        own_copy.start()

    rows = parts * n * ifg_dev
    nifg = n * ifg_dev
    ep = lax.broadcasted_iota(jnp.int32, (NEP, nifg), 0)
    later = (ep == pairs_ref[1:2, :]).astype(F32)
    earlier = (ep == pairs_ref[0:1, :]).astype(F32)
    design = (later - earlier).astype(BF16)
    slot = lax.broadcasted_iota(jnp.int32, (nifg, rows), 1)
    source = slot // (parts * ifg_dev) * ifg_dev + slot % ifg_dev
    spread = (lax.broadcasted_iota(jnp.int32, (nifg, rows), 0) == source).astype(F32).astype(BF16)
    design_half = jnp.dot(design, spread, preferred_element_type=F32).astype(BF16)
    sub = lax.broadcasted_iota(jnp.int32, (NEP, NEP), 0)
    lane = lax.broadcasted_iota(jnp.int32, (NEP, NEP), 1)
    normal = lax.dot_general(design, design, NT, preferred_element_type=F32)
    mat[...] = normal + jnp.where(sub == lane, damping, 0.0)

    def sweep(k):
        m = mat[...]
        col = jnp.sum(jnp.where(lane == k, m, 0.0), axis=1, keepdims=True)
        row = jnp.sum(jnp.where(sub == k, m, 0.0), axis=0, keepdims=True)
        wide_col = jnp.broadcast_to(col, (NEP, NEP))
        pivot = jnp.sum(jnp.where(sub == k, wide_col, 0.0), axis=0, keepdims=True)
        inv = 1.0 / pivot
        scaled = row * inv
        new = m - wide_col * scaled
        new = jnp.where(lane == k, wide_col * inv, new)
        new = jnp.where(sub == k, scaled, new)
        mat[...] = jnp.where((sub == k) & (lane == k), -inv, new)

    strip, wide = 128, 256
    per_line = IMG_W // strip
    turns = 2 * -(-NEP // (lines * per_line))
    swept = min(lines, NEP // (per_line * turns)) * per_line * turns

    slab = npatch // per_line

    def weigh(line):
        here = slice(line * IMG_W, (line + 1) * IMG_W)
        weight[...] = lax.dot_general(
            jnp.ones((EXTRA, LANES), F32),
            wacc[here, :],
            NT,
            precision=lax.Precision.HIGHEST,
            preferred_element_type=F32,
        ).astype(BF16)

    def gather_bound(line, t):
        here = slice(line * IMG_W, (line + 1) * IMG_W)
        cols = pl.ds(pl.multiple_of(t * slab, slab), slab)
        row = jnp.dot(weight[...], jnp.abs(green[here, cols]), preferred_element_type=F32)
        if line > 0:
            row = row + brow[:, cols]
        brow[:, cols] = row

    def generate(line, first, last):
        if line > 0 and first == 0:
            weigh(line - 1)

        @pl.loop(first, last)
        def _(t):
            if line > 0:
                gather_bound(line - 1, t)
            start = pl.multiple_of(line * IMG_W + t * strip, strip)
            mix = feat[pl.ds(start, strip), :]
            spot = t * strip + lax.broadcasted_iota(jnp.int32, (strip, LANES), 0)
            xpos = (2 * spot + 1).astype(F32)
            for q in range(turns):
                if (line + 1) * per_line * turns <= swept:
                    sweep((line * per_line + t) * turns + q)
            total = jnp.zeros((strip, LANES), F32)
            held = None
            for c in range(npatch // wide):
                num = jnp.dot(
                    mix, basis[:, c * wide : (c + 1) * wide], preferred_element_type=F32
                )
                halves = []
                for j in range(wide // LANES):
                    at = slice(c * wide + j * LANES, c * wide + (j + 1) * LANES)
                    away = xpos - prow[0:1, at]
                    inv = lax.rsqrt(away * away + prow[1 + line : 2 + line, at])
                    g = num[:, j * LANES : (j + 1) * LANES] * (inv * inv * inv)
                    halves.append(g.astype(BF16))
                size = jnp.abs(halves[0])
                for piece in halves[1:]:
                    size = size + jnp.abs(piece)
                if held is None:
                    held = size
                else:
                    total = total + (held + size).astype(F32)
                    held = None
                green[pl.ds(start, strip), c * wide : (c + 1) * wide] = jnp.concatenate(halves, 1)
            if held is not None:
                total = total + held.astype(F32)
            wacc[pl.ds(start, strip), :] = total

    def invert():
        @pl.loop(swept, NEP)
        def _(k):
            sweep(k)

        inverse = -mat[...]
        inv_hi = inverse.astype(BF16)
        rest = inverse - inv_hi.astype(F32)
        inv_mid = rest.astype(BF16)
        inv_lo = (rest - inv_mid.astype(F32)).astype(BF16)
        pseudo = (
            jnp.dot(inv_hi, design_half, preferred_element_type=F32)
            + jnp.dot(inv_mid, design_half, preferred_element_type=F32)
            + jnp.dot(inv_lo, design_half, preferred_element_type=F32)
        )
        which = (lax.broadcasted_iota(jnp.int32, (NEP, rows), 1) // ifg_dev) % parts
        if chunks > 1:
            cut = many * ifg_dev
            parted = [jnp.where(half_me == 0, pseudo[:, :cut], pseudo[:, cut:])]
        else:
            parted = [jnp.where(which == h, pseudo, 0.0) for h in range(parts)]
        result = []
        for keep in parted:
            hi = keep.astype(BF16)
            result.append((hi, (keep - hi.astype(F32)).astype(BF16)))
        return result

    def halve(c):
        settle(got.at[c], many - 1, r_x.at[c])
        ((hi, lo),) = pieces
        sums = []
        for part_of in range(2):
            stacked = got[c, :, part_of].reshape(many * ifg_dev, span)
            piece = jnp.dot(hi, stacked, preferred_element_type=F32)
            sums.append(piece + jnp.dot(lo, stacked, preferred_element_type=F32))
        over[c, :, :] = sums[1].astype(BF16)
        pltpu.make_async_remote_copy(
            src_ref=over.at[c],
            dst_ref=back.at[c],
            send_sem=s_m,
            recv_sem=r_m.at[c],
            device_id=ident(mirror),
            device_id_type=mesh_id,
        ).start()
        series[:, c * span : (c + 1) * span] = sums[0]

    ready = min(lines, -(-NEP // (per_line * turns)))
    halved = 0
    for line in range(lines):
        pause = per_line * 3 // 4
        if chunks > 1 and line == lines - 1 and ready <= line:
            generate(line, 0, pause)
            for c in range(halved, chunks):
                halve(c)
            halved = chunks
            generate(line, pause, per_line)
        else:
            generate(line, 0, per_line)
        if line == ready - 1:
            pieces = invert()
        if chunks > 1 and line >= ready - 1:
            upto = chunks if line == lines - 1 else min(line + 1, chunks)
            for c in range(halved, upto):
                halve(c)
            halved = upto

    block = 512
    weigh(lines - 1)

    @pl.loop(0, npatch // slab)
    def _(b):
        gather_bound(lines - 1, b)
        row = brow[:, pl.ds(pl.multiple_of(b * slab, slab), slab)]
        high = row.astype(BF16)
        low = (row - high.astype(F32)).astype(BF16)
        pick = lax.broadcasted_iota(jnp.int32, (EXTRA, slab), 0) == 0
        tail = jnp.where(pick, high.astype(F32), low.astype(F32)).astype(BF16)
        for j in range(slab // LANES):
            bsend[b * (slab // LANES) + j, :, :] = tail[:, j * LANES : (j + 1) * LANES]

    @pl.loop(1, n)
    def _(k):
        d = (me + k) % n
        pltpu.make_async_remote_copy(
            src_ref=bsend.at[d // reps],
            dst_ref=bpart.at[me],
            send_sem=s_b,
            recv_sem=r_b,
            device_id=ident(d),
            device_id_type=mesh_id,
        ).start()

    bpart[me, :, :] = bsend[mine, :, :]

    if chunks == 1:
        own_copy.wait()

    def solve(c):
        if chunks > 1:
            here = slice(c * span, (c + 1) * span)
            pltpu.make_async_copy(back.at[c], back.at[c], r_m.at[c]).wait()
            piece = series[:, here] + back[c].astype(F32)
            series[:, here] = piece
            resid[:, here] = piece.astype(BF16)
            return
        settle(got.at[0], n - 1, r_x.at[0])
        width = npix // parts
        stacked = got[0].reshape(rows, width)
        for h, (hi, lo) in enumerate(pieces):
            piece = jnp.dot(hi, stacked, preferred_element_type=F32)
            piece = piece + jnp.dot(lo, stacked, preferred_element_type=F32)
            series[:, h * width : (h + 1) * width] = piece
            resid[:, h * width : (h + 1) * width] = piece.astype(BF16)

    per_block = block // LANES
    blocks = npatch // block
    first_block = mine // per_block
    side = blocks // 2

    def place(b):
        return (first_block // side + 1 + b // side) % 2 * side + (first_block + 1 + b) % side

    for c in range(chunks - 1):
        solve(c)
        ks = slice(c * span, (c + 1) * span)

        @pl.loop(0, npatch // 1024)
        def _(b):
            cols = pl.ds(pl.multiple_of(b * 1024, 1024), 1024)
            out = jnp.dot(resid[:, ks], green[ks, cols], preferred_element_type=F32)
            if c > 0:
                out = out + guess[:, cols]
            guess[:, cols] = out

    solve(chunks - 1)

    def product(at, first):
        cols = pl.ds(pl.multiple_of(at * block, block), block)
        if first and chunks > 1:
            ks = slice((chunks - 1) * span, npix)
            out = jnp.dot(resid[:, ks], green[ks, cols], preferred_element_type=F32)
            return out + guess[:, cols]
        return jnp.dot(resid[...], green[:, cols], preferred_element_type=F32)

    def bounds():
        settle(bpart, n - 1, r_b)
        settle(bpart, n - 1, s_b)
        both = lax.fori_loop(
            1, n, lambda d, acc: acc + bpart[d].astype(F32), bpart[0].astype(F32)
        )
        return both[0:1] + both[1:2]

    def project(part, recv_sem, pair, pair_sem, first):
        @pl.loop(0, blocks)
        def _(b):
            at = place(b)
            half_out = product(at, first).astype(BF16)
            for j in range(per_block):
                send[at * per_block + j, :, :] = half_out[:, j * LANES : (j + 1) * LANES]
            for j in range(per_block):
                group = at * per_block + j
                for r in range(reps):
                    d = group * reps + r

                    @pl.when(d != me)
                    def _():
                        pltpu.make_async_remote_copy(
                            src_ref=send.at[group],
                            dst_ref=part.at[me],
                            send_sem=s_p,
                            recv_sem=recv_sem,
                            device_id=ident(d),
                            device_id_type=mesh_id,
                        ).start()

        part[me, :, :] = send[mine, :, :]
        settle(part, n - 1, recv_sem)
        settle(part, n - 1, s_p)
        bound = bounds() if first else None
        total = lax.fori_loop(
            1, n, lambda d, acc: acc + part[d].astype(F32), part[0].astype(F32)
        )
        return total, bound

    chips = n // 2
    per_pair = per_block // 2

    def project_split(part, recv_sem, pair, pair_sem, first):
        def forward(at):
            here = pl.ds(at * per_pair, per_pair)
            pltpu.make_async_copy(pair.at[here], pair.at[here], pair_sem.at[at]).wait()
            for j in range(per_pair):
                slot = at * per_pair + j
                send[slot, :, :] = (own[slot] + pair[slot].astype(F32)).astype(BF16)
            for j in range(per_pair):
                slot = at * per_pair + j

                @pl.when(slot != chip)
                def _():
                    pltpu.make_async_remote_copy(
                        src_ref=send.at[slot],
                        dst_ref=part.at[chip],
                        send_sem=s_p,
                        recv_sem=recv_sem,
                        device_id=ident(slot * 2 + core),
                        device_id_type=mesh_id,
                    ).start()

        @pl.loop(0, blocks)
        def _(b):
            at = place(b)
            out = product(at, first)
            for j in range(per_pair):
                even = out[:, 2 * j * LANES : (2 * j + 1) * LANES]
                odd = out[:, (2 * j + 1) * LANES : (2 * j + 2) * LANES]
                slot = at * per_pair + j
                own[slot, :, :] = jnp.where(core == 0, even, odd)
                half[slot, :, :] = jnp.where(core == 0, odd, even).astype(BF16)
            here = pl.ds(at * per_pair, per_pair)
            pltpu.make_async_remote_copy(
                src_ref=half.at[here],
                dst_ref=pair.at[here],
                send_sem=s_h,
                recv_sem=pair_sem.at[at],
                device_id=ident(partner),
                device_id_type=mesh_id,
            ).start()

            @pl.when(b > 0)
            def _():
                forward(place(b - 1))

        forward(place(blocks - 1))
        part[chip, :, :] = send[chip, :, :]
        settle(half, chips, s_h)
        bound = bounds() if first else None
        settle(part, chips - 1, recv_sem)
        settle(part, chips - 1, s_p)
        total = lax.fori_loop(
            1, chips, lambda d, acc: acc + part[d].astype(F32), part[0].astype(F32)
        )
        return total, bound

    tile = 512

    def share(slip, gath, recv_sem, pass_sem, target):
        gath[mine, :, :] = slip.astype(BF16)

        @pl.loop(1, gathered)
        def _(k):
            d = (me + (n - k * reps)) % n
            pltpu.make_async_remote_copy(
                src_ref=gath.at[mine],
                dst_ref=gath.at[mine],
                send_sem=s_g,
                recv_sem=recv_sem.at[first_block],
                device_id=ident(d),
                device_id_type=mesh_id,
            ).start()

        for i in range(blocks):
            at = (first_block + i) % blocks
            settle(gath, per_block - 1 if i == 0 else per_block, recv_sem.at[at])
            for j in range(per_block):
                full[:, j * LANES : (j + 1) * LANES] = gath[at * per_block + j]
            cols = pl.ds(pl.multiple_of(at * block, block), block)

            @pl.loop(0, npix // tile)
            def _(t):
                here = pl.ds(pl.multiple_of(t * tile, tile), tile)
                out = lax.dot_general(
                    full[:, 0:block], green[here, cols], NT, preferred_element_type=F32
                )
                if i > 0:
                    out = target[:, here] + out
                target[:, here] = out

        settle(gath, gathered - 1, s_g)

    each = chips // batches
    home = chip // each
    span_at = 2 * each * LANES

    def share_split(slip, gath, recv_sem, pass_sem, target):
        mine_at = core * chips + chip
        gath[mine_at, :, :] = slip.astype(BF16)

        def give(to, side_core):
            pltpu.make_async_remote_copy(
                src_ref=gath.at[mine_at],
                dst_ref=gath.at[mine_at],
                send_sem=s_g,
                recv_sem=recv_sem.at[home],
                device_id=ident(to * 2 + side_core),
                device_id_type=mesh_id,
            ).start()

        give(chip, 1 - core)
        for k in range(1, each):
            to = home * each + (chip + k) % each
            give(to, core)
            give(to, 1 - core)

        def order(i):
            if batches != 4:
                return (home + i) % batches
            low, high = i % 2, i // 2
            bit = home % 2
            near = bit + low - 2 * bit * low
            far = home // 2 + high - 2 * (home // 2) * high
            return 2 * far + near

        @pl.loop(1, batches)
        def _(i):
            for k in range(each):
                give(order(i) * each + (chip + k) % each, core)

        def passing(at):
            return pl.ds(core * chips + at * each, each)

        def collect(i):
            at = order(i)
            settle(gath, each, recv_sem.at[at])
            pltpu.make_async_remote_copy(
                src_ref=gath.at[passing(at)],
                dst_ref=gath.at[passing(at)],
                send_sem=s_f,
                recv_sem=pass_sem.at[at],
                device_id=ident(partner),
                device_id_type=mesh_id,
            ).start()

        target[:, 0:npix] = jnp.zeros((NEP, npix), F32)

        @pl.loop(0, batches)
        def _(i):
            at = order(i)

            @pl.when(i == 0)
            def _():
                settle(gath, 2 * each - 1, recv_sem.at[at])

            @pl.when(i > 0)
            def _():
                settle(gath, each, pass_sem.at[at])

            for j in range(each):
                for p in range(2):
                    lane = (2 * j + p) * LANES
                    full[:, lane : lane + LANES] = gath[p * chips + at * each + j]
            tall[...] = full[:, 0:span_at].T

            @pl.when(i + 1 < batches)
            def _():
                collect(i + 1)

            for start in range(0, npix, 1024):
                flat = slice(start, start + 512)
                long = slice(start + 512, start + 1024)
                wide_out = long_out = None
                for k in range(0, span_at, 256):
                    ks = slice(k, k + 256)
                    cols = pl.ds(pl.multiple_of(at * span_at + k, 256), 256)
                    a = lax.dot_general(
                        full[:, ks], green[flat, cols], NT, preferred_element_type=F32
                    )
                    b = jnp.dot(green[long, cols], tall[ks, :], preferred_element_type=F32)
                    wide_out = a if wide_out is None else wide_out + a
                    long_out = b if long_out is None else long_out + b
                target[:, flat] = target[:, flat] + wide_out
                target[:, long] = target[:, long] + long_out.T

        settle(gath, 2 * each - 1 + (batches - 1) * each, s_g)
        settle(gath, (batches - 1) * each, s_f)

    if split:
        project, share = project_split, share_split
    sums, bound = project(part_a, r_pa, pair_a, r_ha, True)
    if chunks > 1:
        for c in range(chunks):
            settle(got.at[c], many - 1, s_x)
        settle(over, chunks, s_m)
    else:
        settle(got.at[0], n - 1, s_x)
    slip = sums / bound
    share(slip, gath_a, r_ga, r_fa, guess)
    resid[...] = (series[...] - guess[:, 0:npix]).astype(BF16)
    slip = slip + project(part_b, r_pb, pair_b, r_hb, False)[0] / bound
    slip_ref[...] = slip
    share(slip, gath_b, r_gb, r_fb, pred_ref)


def on_device(interferograms, epoch_pairs, los, patch_place, patch_depth):
    n = lax.axis_size(("pix", "rep"))
    me = lax.axis_index(("pix", "rep"))
    ifg_dev, total = interferograms.shape
    npix = total // n
    npatch = patch_depth.shape[0]
    own = npatch // n
    reps = max(LANES // own, 1)
    parts = max(16 // ifg_dev, 1)
    width = npix // parts
    lines = npix // IMG_W

    chunks = 1
    if ifg_dev % 8 == 0 and lines > 1:
        chunks, parts, width = lines, 1, IMG_W
        xs = interferograms
    else:
        xs = interferograms.astype(BF16).reshape(ifg_dev, n, parts, width)
        xs = xs.transpose(1, 2, 0, 3).reshape(n, parts * ifg_dev, width)
    inside = chunks > 1
    swap = (chunks, n // 2, 2, ifg_dev, width)
    groups = npatch // LANES
    cfg = (n, reps, npix, npatch, parts, ifg_dev, lines, chunks)
    chips = n // 2
    pairs = chips if reps == 1 else 1
    small = (1,) + (16, LANES)
    loads = 8 if n % 8 == 0 else 1
    batches = max(n // 8, 1)
    vmem = pl.BlockSpec(memory_space=pltpu.VMEM)
    piece = (NEP, LANES)
    block = 512
    dma = pltpu.SemaphoreType.DMA
    predicted, slip = pl.pallas_call(
        functools.partial(kernel, cfg),
        out_shape=(
            pltpu.VMEM((NEP, npix), F32),
            pltpu.VMEM((NEP, LANES), F32),
        ),
        in_specs=[vmem, vmem, vmem, vmem, pl.BlockSpec(memory_space=pl.ANY)],
        out_specs=(vmem, vmem),
        scratch_shapes=[
            pltpu.VMEM((npix, 32), BF16),
            pltpu.VMEM((32, npatch), BF16),
            pltpu.VMEM((1 + lines, npatch), F32),
            pltpu.VMEM((NEP, NEP), F32),
            pltpu.VMEM((npix, npatch), BF16),
            pltpu.VMEM((npix, LANES), F32),
            pltpu.VMEM((EXTRA, IMG_W), BF16),
            pltpu.VMEM((EXTRA, npatch), F32),
            pltpu.VMEM(swap if inside else (1, n, parts * ifg_dev, width), BF16),
            pltpu.VMEM((NEP, npix), F32),
            pltpu.VMEM((NEP, npix), BF16),
            pltpu.VMEM((groups, EXTRA, LANES), BF16),
            pltpu.VMEM((n, EXTRA, LANES), BF16),
            pltpu.VMEM((groups,) + piece, BF16),
            pltpu.VMEM((n,) + piece, BF16),
            pltpu.VMEM((n,) + piece, BF16),
            pltpu.VMEM((groups, NEP, LANES), BF16),
            pltpu.VMEM((groups, NEP, LANES), BF16),
            pltpu.VMEM((NEP, max(block, 2 * LANES * chips // batches)), BF16),
            pltpu.VMEM((2 * LANES * chips // batches, NEP), BF16),
            pltpu.VMEM((NEP, max(npix, npatch)), F32),
            pltpu.VMEM(interferograms.shape if inside else (8, LANES), F32),
            pltpu.VMEM(swap if inside else small, BF16),
            pltpu.VMEM((chunks, NEP, width) if inside else small, BF16),
            pltpu.VMEM((chunks, NEP, width) if inside else small, BF16),
            pltpu.VMEM((pairs,) + piece, F32),
            pltpu.VMEM((pairs,) + piece, BF16),
            pltpu.VMEM((pairs,) + piece, BF16),
            pltpu.VMEM((pairs,) + piece, BF16),
            dma,
            dma((chunks,)),
            dma((loads,)),
            dma,
            dma((chunks,)),
            dma,
            dma,
            dma,
            dma,
            dma,
            dma,
            dma((npatch // block,)),
            dma((npatch // block,)),
            dma,
            dma((max(npatch // block, batches),)),
            dma((max(npatch // block, batches),)),
            dma,
            dma((batches,)),
            dma((batches,)),
        ],
        compiler_params=pltpu.CompilerParams(
            collective_id=0, has_side_effects=True, vmem_limit_bytes=59 * 1024 * 1024
        ),
    )(epoch_pairs, los, patch_place, patch_depth[None], xs)
    if reps > 1:
        slip = lax.dynamic_slice_in_dim(slip, (me % reps) * own, own, 1)
    return (predicted, slip)


def solution(mesh):
    placed = (P(("pix", "rep"), None), P(), P(None, ("pix", "rep")), P(), P())
    return jax.shard_map(
        on_device,
        mesh=mesh,
        in_specs=placed,
        out_specs=(P(None, ("pix", "rep")), P(None, ("pix", "rep"))),
        check_vma=False,
    )
```
